256 devices in a mesh: gx: 16 (over y_hi, z), gy: 16 (over y_lo, x, core).
Axes of the slice: x: 4, y: 4 (y_hi: 2, y_lo: 2; y = y_hi * 2 + y_lo), z: 8, core: 2. Of those that a mesh axis runs over, the one named last changes fastest.
Arguments:
- hidden: bfloat16 [8192, 14336], P('gx', 'gy'), may hold values from -6 to 6
- weight: bfloat16 [4096, 14336], P(None, 'gy'), may hold values from -0.0625 to 0.0625
- cotangent: bfloat16 [8192, 4096], P('gx', 'gy'), may hold values from -6 to 6
Outputs:
- output: bfloat16 [8192, 4096], P('gx', 'gy')
- hidden_grad: bfloat16 [8192, 14336], P('gx', 'gy')
- weight_grad: float32 [4096, 14336], P('gx', 'gy')
The draws below stay inside these ranges and needn't reach their ends.
All inputs are finite; a program needn't handle non-finite values.
Results may differ from the reference program's by a relative error of at most 0.001.
Values may be sent and summed in bfloat16 or wider, within the bound.
A program may use at most 128 MiB of HBM per device.

```python
import jax
import jax.numpy as jnp

D = 4096
FF = 14336
TOKENS = 8192


def strengthened(values, rng, source, target, blocks, factor):
    def block_of(position):
        return (jnp.arange(values.shape[position]) // (values.shape[position] // blocks)).reshape((-1,) + (1,) * (values.ndim - 1 - position))

    near = jax.random.permutation(rng, blocks)[block_of(target)]
    far = (block_of(target) + blocks // 2) % blocks
    return jnp.where((block_of(source) == near) | (block_of(source) == far), factor * values, values)


def block_scale(rng, dims, pieces, smallest, high):
    gain, own = 1.0, jax.random.fold_in(rng, 6)
    for position, blocks in pieces:
        heights = jnp.exp(jax.random.uniform(jax.random.fold_in(own, position), (blocks,), jnp.float32, smallest / len(pieces), high / len(pieces)))
        gain = gain * jnp.repeat(heights, dims[position] // blocks).reshape([-1 if axis == position else 1 for axis in range(len(dims))])
    return gain


def scatter_about(own_key, dims, spread, limit, shards=(), held_as=jnp.bfloat16):
    loudness = block_scale(own_key, dims, shards, -0.22, 0.18) if shards else 1.0
    values = jax.random.normal(own_key, dims, jnp.float32) * spread * loudness
    return jnp.minimum(jnp.maximum(values, -limit), limit).astype(held_as)


def gaussian_with(stream_key, shape, deviation, reach, split, heavy, kind=jnp.bfloat16):
    result = deviation * jax.random.normal(stream_key, shape, jnp.float32)
    if split:
        result = result * block_scale(stream_key, shape, split, -0.22, 0.18)
    return jnp.clip(strengthened(result, jax.random.fold_in(stream_key, 3), *heavy), -reach, reach).astype(kind)


def setup_inputs(seed: int = 0) -> dict:
    arg_keys = jax.random.split(jax.random.key(seed), 4)
    hidden = scatter_about(arg_keys[0], (TOKENS, FF), 1.0, 6.0, ((0, 16), (1, 16)))
    weight = gaussian_with(arg_keys[1], (D, FF), FF ** -0.5, 0.0625, ((1, 16),), (1, 0, 16, 2.0))
    cotangent = gaussian_with(arg_keys[2], (TOKENS, D), 1.0, 6.0, ((0, 16), (1, 16)), (0, 1, 16, 2.0))
    return {"hidden": hidden, "weight": weight, "cotangent": cotangent}


def reference(hidden, weight, cotangent):
    hidden_f = hidden.astype(jnp.float32)
    weight_f = weight.astype(jnp.float32)
    cotangent_f = cotangent.astype(jnp.float32)
    output = jnp.dot(hidden_f, weight_f.T, preferred_element_type=jnp.float32).astype(jnp.bfloat16)
    hidden_grad = jnp.dot(cotangent_f, weight_f, preferred_element_type=jnp.float32).astype(jnp.bfloat16)
    weight_grad = jnp.dot(cotangent_f.T, hidden_f, preferred_element_type=jnp.float32) * (TOKENS ** -0.5)
    return output, hidden_grad, weight_grad
```

```python
import functools

import jax
import jax.numpy as jnp
from jax import lax
from jax.experimental import pallas as pl
from jax.experimental.pallas import tpu as pltpu
from jax.sharding import PartitionSpec as P

MESH = pl.DeviceIdType.MESH
F32 = jnp.float32
BF16 = jnp.bfloat16
NX, NZ = 4, 8
HCH = 4
WCH = 4


def zigzag(i, top):
    odd = lax.rem(i, 2)
    return top + (1 - odd) * (i // 2) - odd * ((i + 1) // 2)


def kernel(
    scale,
    hidden,
    weight,
    cotangent,
    output,
    hidden_grad,
    weight_grad,
    w,
    hid,
    hrel,
    cot,
    o_send,
    o_sum,
    xh,
    xf,
    yb,
    part,
    zb,
    acc,
    hgb,
    outb,
    load_sem,
    store_sem,
    cy_s,
    cy_r,
    cx_s,
    cx_r,
    cd_s,
    cd_r,
    h_s,
    h_r,
    o_s,
    o_r,
    xo_s,
    xo_r,
    yo_s,
    yo_r,
    z_s,
    z_r,
):
    gx = lax.axis_index("gx")
    gy = lax.axis_index("gy")
    y_hi, z = gx // NZ, lax.rem(gx, NZ)
    c = lax.rem(gy, 2)
    x = lax.rem(gy // 2, NX)
    y_lo = gy // (2 * NX)
    tok, ff = hid.shape[1], hid.shape[2]
    feat = cot.shape[2]
    half = tok // 2
    rows = feat // 2

    def dev(yh, yl, xx, zz, cc):
        return (yh * NZ + zz, (yl * NX + xx) * 2 + cc)

    right, left = lax.rem(x + 1, NX), lax.rem(x + NX - 1, NX)
    across = lax.rem(x + 2, NX)
    core = dev(y_hi, y_lo, x, z, 1 - c)
    near = dev(y_hi, 1 - y_lo, x, z, c)
    far = dev(1 - y_hi, 1 - y_lo, x, z, c)
    first = dev(lax.rem(y_hi + c, 2), 1 - y_lo, x, z, c)
    second = dev(lax.rem(y_hi + 1 - c, 2), 1 - y_lo, x, z, c)
    x_dev = (dev(y_hi, y_lo, right, z, c), dev(y_hi, y_lo, left, z, c))
    z_dev = (
        dev(y_hi, y_lo, x, lax.rem(z + 1, NZ), c),
        dev(y_hi, y_lo, x, lax.rem(z + NZ - 1, NZ), c),
    )

    def rc(src, dst, ss, rs, to):
        return pltpu.make_async_remote_copy(
            src_ref=src, dst_ref=dst, send_sem=ss, recv_sem=rs, device_id=to, device_id_type=MESH
        )

    sent = []

    def go(copy):
        copy.start()
        sent.append(copy)

    base = (y_lo * NX * 2, (1 - y_lo) * NX * 2, 16)

    def slot(kind, xx):
        return cot.at[base[kind] + xx * 2 + c]

    mine = slot(0, x)
    ld_cot = pltpu.make_async_copy(cotangent, mine, load_sem.at[0])
    ld_hid = pltpu.make_async_copy(hidden, hid.at[0], load_sem.at[1])
    ld_cot.start()
    ld_hid.start()
    wrows = w.shape[0] // WCH
    ld_w = [
        pltpu.make_async_copy(
            weight.at[pl.ds(i * wrows, wrows)], w.at[pl.ds(i * wrows, wrows)], load_sem.at[2 + i]
        )
        for i in range(WCH)
    ]
    for copy in ld_w:
        copy.start()

    barrier = pltpu.get_barrier_semaphore()
    peers = (core, near, far, *x_dev, *z_dev)
    for peer in peers:
        pl.semaphore_signal(barrier, inc=1, device_id=peer, device_id_type=MESH)
    pl.semaphore_wait(barrier, len(peers))

    def xs_full(kind, d):
        return rc(slot(kind, x), slot(kind, x), cx_s.at[kind, d], cx_r.at[kind, d], x_dev[d])

    def xs_half(kind, d):
        src = slot(kind, (left, right)[d]).at[pl.ds(d * half, half)]
        return rc(src, src, cx_s.at[kind, 2 + d], cx_r.at[kind, 2 + d], x_dev[d])

    def from_full(kind, d):
        ref = slot(kind, (left, right)[d])
        return rc(ref, ref, cx_s.at[kind, d], cx_r.at[kind, d], x_dev[d])

    def from_half(kind, d):
        ref = slot(kind, across).at[pl.ds(d * half, half)]
        return rc(ref, ref, cx_s.at[kind, 2 + d], cx_r.at[kind, 2 + d], x_dev[d])

    def to_core(kind, j):
        ref = slot(kind, (x, left, right, across)[j])
        return rc(ref, ref, cd_s.at[kind, j], cd_r.at[kind, j], core)

    def from_core(kind, j):
        ref = cot.at[base[kind] + (x, left, right, across)[j] * 2 + 1 - c]
        return rc(ref, ref, cd_s.at[kind, j], cd_r.at[kind, j], core)

    def spread(kind):
        go(xs_full(kind, 0))
        go(xs_full(kind, 1))
        go(to_core(kind, 0))

    def relay(kind):
        for d in range(2):
            from_full(kind, d).wait_recv()
            go(xs_half(kind, d))
        go(to_core(kind, 1))
        go(to_core(kind, 2))

    def finish(kind):
        for d in range(2):
            from_half(kind, d).wait_recv()
        go(to_core(kind, 3))

    ld_cot.wait()
    near_slot, far_slot = slot(1, x), slot(2, x)
    go(rc(mine, near_slot_of(cot, y_lo, x, c), cy_s.at[0], cy_r.at[0], near))
    middle = y_hi != y_lo

    @pl.when(middle)
    def _():
        rc(mine, far_slot, cy_s.at[1], cy_r.at[1], far).start()

    spread(0)

    hrows = tok // HCH

    def hpiece(ref, i):
        return ref.at[pl.ds(i * hrows, hrows)]

    ld_hid.wait()
    for i in range(HCH):
        go(rc(hpiece(hid.at[0], i), hpiece(hrel, i), h_s.at[0, i], h_r.at[0, i], first))

    def hrelay(i):
        ref = hpiece(hrel, i)
        rc(ref, ref, h_s.at[0, i], h_r.at[0, i], first).wait_recv()
        go(rc(ref, hpiece(hid.at[1], i), h_s.at[1, i], h_r.at[1, i], second))

    def out_part(t, cc):
        yp = lax.rem(y_lo + 1 + lax.rem(t, 2), 2)
        g = (yp * NX + lax.rem(x + zigzag(t // 2, 2), NX)) * 2 + cc
        wg = w[pl.ds(pl.multiple_of(g * feat, feat), feat), :]
        return lax.dot_general(hid[0], wg, (((1,), (1,)), ((), ())), preferred_element_type=F32)

    def o_copy(t):
        return rc(o_send.at[t], o_sum.at[t], o_s.at[t], o_r.at[t], core)

    for copy in ld_w:
        copy.wait()

    def send_out(t, _):
        o_send[t] = out_part(t, 1 - c)
        o_copy(t).start()
        return 0

    lax.fori_loop(0, 4, send_out, 0)

    rc(near_slot, near_slot, cy_s.at[0], cy_r.at[0], near).wait_recv()

    @pl.when(jnp.logical_not(middle))
    def _():
        rc(near_slot, far_slot, cy_s.at[1], cy_r.at[1], far).start()

    spread(1)
    hrelay(0)
    relay(0)
    lax.fori_loop(4, 8, send_out, 0)
    hrelay(1)
    rc(far_slot, far_slot, cy_s.at[1], cy_r.at[1], far).wait_recv()
    spread(2)
    relay(1)
    hrelay(2)

    def add_out(t, _):
        o_copy(t).wait_recv()
        o_sum[t] = o_sum[t] + out_part(t, c)
        return 0

    lax.fori_loop(0, 8, add_out, 0)
    finish(0)
    hrelay(3)
    relay(2)
    finish(1)

    def xo_half(d, q):
        src = o_sum.at[q].at[pl.ds(d * half, half)]
        return rc(src, xh.at[d, q], xo_s.at[0, d, q], xo_r.at[0, d, q], x_dev[d])

    def xo_full(d, q):
        return rc(o_sum.at[2 + 2 * d + q], xf.at[d, q], xo_s.at[1, d, q], xo_r.at[1, d, q], x_dev[d])

    finish(2)
    for q in range(2):
        for d in range(2):
            go(xo_half(d, q))
    for kind in range(3):
        for j in range(4):
            from_core(kind, j).wait_recv()
    for i in range(HCH):
        ref = hpiece(hid.at[1], i)
        rc(ref, ref, h_s.at[1, i], h_r.at[1, i], second).wait_recv()

    def w_part(i, _):
        zz = lax.rem(z + zigzag(i, 4), NZ)
        dims = (((0,), (0,)), ((), ()))
        part[i] = lax.dot_general(
            cot[y_hi * NZ + zz], hid[0], dims, preferred_element_type=F32
        ) + lax.dot_general(cot[16 + zz], hid[1], dims, preferred_element_type=F32)
        return 0

    index_of = {4: 0, 3: 1, 5: 2, 2: 3, 6: 4, 1: 5, 7: 6, 0: 7}

    def z_part(d, m):
        k = 4 - (m + 1) // 2
        piece = (m + d) % 2
        return part.at[index_of[(k if d == 0 else -k) % NZ]].at[pl.ds(piece * rows, rows)]

    def z_copy(d, m):
        src = z_part(d, m) if m < 2 else zb.at[d, m - 2]
        return rc(src, zb.at[d, m], z_s.at[d, m], z_r.at[d, m], z_dev[d])

    def z_step(m):
        for d in range(2):
            z_copy(d, m - 2).wait_recv()
            zb[d, m - 2] = zb[d, m - 2] + z_part(d, m)[...]
            go(z_copy(d, m))

    lax.fori_loop(0, 3, w_part, 0)
    for m in range(2):
        for d in range(2):
            go(z_copy(d, m))
    lax.fori_loop(3, 8, w_part, 0)

    def h_part(g, _):
        acc[...] = acc[...] + jnp.dot(
            cot[g], w[pl.ds(pl.multiple_of(g * feat, feat), feat), :], preferred_element_type=F32
        )
        return 0

    acc[...] = jnp.dot(cot[0], w[pl.ds(0, feat), :], preferred_element_type=F32)
    lax.fori_loop(1, 16, h_part, 0)
    hgb[...] = acc[...].astype(BF16)
    st_hg = pltpu.make_async_copy(hgb, hidden_grad, store_sem.at[0])
    st_hg.start()

    def xo_add(q):
        xo_half(0, q).wait_recv()
        o_sum[2 + q, pl.ds(0, half)] = o_sum[2 + q, pl.ds(0, half)] + xh[0, q]
        go(xo_full(0, q))
        xo_half(1, q).wait_recv()
        o_sum[4 + q, pl.ds(half, half)] = o_sum[4 + q, pl.ds(half, half)] + xh[1, q]
        go(xo_full(1, q))

    def xo_end(q):
        for d in range(2):
            xo_full(d, q).wait_recv()
        o_sum[6 + q] = o_sum[6 + q] + xf[0, q] + xf[1, q]

    yo = rc(o_sum.at[6], yb, yo_s.at[0], yo_r.at[0], near)
    z_step(2)
    xo_add(0)
    xo_add(1)
    z_step(3)
    z_step(4)
    xo_end(0)
    go(yo)
    z_step(5)
    xo_end(1)
    z_step(6)
    yo.wait_recv()
    outb[...] = (o_sum[7] + yb[...]).astype(BF16)
    st_out = pltpu.make_async_copy(outb, output, store_sem.at[1])
    st_out.start()

    z_copy(0, 5).wait_recv()
    z_copy(1, 5).wait_recv()
    z_copy(0, 6).wait_recv()
    z_copy(1, 6).wait_recv()
    part[7, pl.ds(0, rows)] = (part[7, pl.ds(0, rows)] + zb[0, 6] + zb[1, 5]) * scale
    part[7, pl.ds(rows, rows)] = (part[7, pl.ds(rows, rows)] + zb[0, 5] + zb[1, 6]) * scale
    st_wg = pltpu.make_async_copy(part.at[7], weight_grad, store_sem.at[2])
    st_wg.start()

    rc(mine, far_slot, cy_s.at[1], cy_r.at[1], far).wait_send()

    def sent_out(t, _):
        o_copy(t).wait_send()
        return 0

    lax.fori_loop(0, 8, sent_out, 0)
    for copy in sent:
        copy.wait_send()
    st_hg.wait()
    st_out.wait()
    st_wg.wait()


def near_slot_of(cot, y_lo, x, c):
    return cot.at[y_lo * NX * 2 + x * 2 + c]


def shards(hidden, weight, cotangent):
    tok, ff = hidden.shape
    d_all = weight.shape[0]
    feat = cotangent.shape[1]
    scale = float(tok * lax.axis_size("gx")) ** (-0.5)
    any_space = pl.BlockSpec(memory_space=pl.ANY)
    sem = pltpu.SemaphoreType.DMA
    v = pltpu.VMEM
    return pl.pallas_call(
        functools.partial(kernel, scale),
        out_shape=(
            jax.ShapeDtypeStruct((tok, feat), BF16),
            jax.ShapeDtypeStruct((tok, ff), BF16),
            jax.ShapeDtypeStruct((feat, ff), F32),
        ),
        in_specs=[any_space] * 3,
        out_specs=(any_space,) * 3,
        scratch_shapes=[
            v((d_all, ff), BF16),
            v((2, tok, ff), BF16),
            v((tok, ff), BF16),
            v((24, tok, feat), BF16),
            v((8, tok, feat), F32),
            v((8, tok, feat), F32),
            v((2, 2, tok // 2, feat), F32),
            v((2, 2, tok, feat), F32),
            v((tok, feat), F32),
            v((8, feat, ff), F32),
            v((2, 7, feat // 2, ff), F32),
            v((tok, ff), F32),
            v((tok, ff), BF16),
            v((tok, feat), BF16),
            sem((2 + WCH,)),
            sem((3,)),
            sem((2,)),
            sem((2,)),
            sem((3, 4)),
            sem((3, 4)),
            sem((3, 4)),
            sem((3, 4)),
            sem((2, HCH)),
            sem((2, HCH)),
            sem((8,)),
            sem((8,)),
            sem((2, 2, 2)),
            sem((2, 2, 2)),
            sem((1,)),
            sem((1,)),
            sem((2, 7)),
            sem((2, 7)),
        ],
        compiler_params=pltpu.CompilerParams(
            collective_id=0, has_side_effects=True, vmem_limit_bytes=62 * 1024 * 1024
        ),
    )(hidden, weight, cotangent)


def solution(mesh):
    placed = (P("gx", "gy"), P(None, "gy"), P("gx", "gy"))
    return jax.shard_map(
        shards,
        mesh=mesh,
        in_specs=placed,
        out_specs=(P("gx", "gy"), P("gx", "gy"), P("gx", "gy")),
        check_vma=False,
    )
```

```python
import functools

import jax
import jax.numpy as jnp
from jax import lax
from jax.experimental import pallas as pl
from jax.experimental.pallas import tpu as pltpu
from jax.sharding import PartitionSpec as P

MESH = pl.DeviceIdType.MESH
F32 = jnp.float32
BF16 = jnp.bfloat16
NX, NZ = 4, 8
HCH = 4
WCH = 4
ZR = 16


def zigzag(i, top):
    odd = lax.rem(i, 2)
    return top + (1 - odd) * (i // 2) - odd * ((i + 1) // 2)


def kernel(
    scale,
    hidden,
    weight,
    cotangent,
    output,
    hidden_grad,
    weight_grad,
    w,
    hid,
    hrel,
    cot,
    o_send,
    o_sum,
    xh,
    xf,
    yb,
    part,
    zs,
    zb,
    acc,
    hgb,
    outb,
    load_sem,
    store_sem,
    cy_s,
    cy_r,
    cx_s,
    cx_r,
    cd_s,
    cd_r,
    h_s,
    h_r,
    o_s,
    o_r,
    xo_s,
    xo_r,
    yo_s,
    yo_r,
    z_s,
    z_r,
):
    gx = lax.axis_index("gx")
    gy = lax.axis_index("gy")
    y_hi, z = gx // NZ, lax.rem(gx, NZ)
    c = lax.rem(gy, 2)
    x = lax.rem(gy // 2, NX)
    y_lo = gy // (2 * NX)
    tok, ff = hid.shape[1], hid.shape[2]
    feat = cot.shape[2]
    half = tok // 2
    rows = feat // 2

    def dev(yh, yl, xx, zz, cc):
        return (yh * NZ + zz, (yl * NX + xx) * 2 + cc)

    right, left = lax.rem(x + 1, NX), lax.rem(x + NX - 1, NX)
    across = lax.rem(x + 2, NX)
    core = dev(y_hi, y_lo, x, z, 1 - c)
    near = dev(y_hi, 1 - y_lo, x, z, c)
    far = dev(1 - y_hi, 1 - y_lo, x, z, c)
    first = dev(lax.rem(y_hi + c, 2), 1 - y_lo, x, z, c)
    second = dev(lax.rem(y_hi + 1 - c, 2), 1 - y_lo, x, z, c)
    x_dev = (dev(y_hi, y_lo, right, z, c), dev(y_hi, y_lo, left, z, c))
    z_dev = (
        dev(y_hi, y_lo, x, lax.rem(z + 1, NZ), c),
        dev(y_hi, y_lo, x, lax.rem(z + NZ - 1, NZ), c),
    )

    def rc(src, dst, ss, rs, to):
        return pltpu.make_async_remote_copy(
            src_ref=src, dst_ref=dst, send_sem=ss, recv_sem=rs, device_id=to, device_id_type=MESH
        )

    sent = []

    def go(make, *where):
        make(*where).start()
        sent.append((make, where))

    base = (y_hi * NX * 2, (1 - y_hi) * NX * 2, 16)
    middle = lax.rem(y_hi + y_lo, 2)

    def slot(kind, xx):
        return cot.at[base[kind] + xx * 2 + c]

    mine = cot.at[y_lo * NX * 2 + x * 2 + c]
    near_slot = cot.at[(1 - y_lo) * NX * 2 + x * 2 + c]
    far_slot = slot(2, x)
    ld_cot = pltpu.make_async_copy(cotangent, mine, load_sem.at[0])
    ld_hid = pltpu.make_async_copy(hidden, hid.at[0], load_sem.at[1])
    ld_cot.start()
    ld_hid.start()
    wrows = w.shape[0] // WCH
    ld_w = [
        pltpu.make_async_copy(
            weight.at[pl.ds(i * wrows, wrows)], w.at[pl.ds(i * wrows, wrows)], load_sem.at[2 + i]
        )
        for i in range(WCH)
    ]
    for copy in ld_w:
        copy.start()

    barrier = pltpu.get_barrier_semaphore()
    peers = (core, near, far, *x_dev, *z_dev)
    for peer in peers:
        pl.semaphore_signal(barrier, inc=1, device_id=peer, device_id_type=MESH)
    pl.semaphore_wait(barrier, len(peers))

    def xs_full(kind, d):
        return rc(slot(kind, x), slot(kind, x), cx_s.at[kind, d], cx_r.at[kind, d], x_dev[d])

    def xs_half(kind, d):
        src = slot(kind, (left, right)[d]).at[pl.ds(d * half, half)]
        return rc(src, src, cx_s.at[kind, 2 + d], cx_r.at[kind, 2 + d], x_dev[d])

    def from_full(kind, d):
        ref = slot(kind, (left, right)[d])
        return rc(ref, ref, cx_s.at[kind, d], cx_r.at[kind, d], x_dev[d])

    def from_half(kind, d):
        ref = slot(kind, across).at[pl.ds(d * half, half)]
        return rc(ref, ref, cx_s.at[kind, 2 + d], cx_r.at[kind, 2 + d], x_dev[d])

    def to_core(kind, j):
        ref = slot(kind, (x, left, right, across)[j])
        return rc(ref, ref, cd_s.at[kind, j], cd_r.at[kind, j], core)

    def from_core(kind, j):
        ref = cot.at[base[kind] + (x, left, right, across)[j] * 2 + 1 - c]
        return rc(ref, ref, cd_s.at[kind, j], cd_r.at[kind, j], core)

    def to_near():
        return rc(mine, mine, cy_s.at[0], cy_r.at[0], near)

    def from_near():
        return rc(near_slot, near_slot, cy_s.at[0], cy_r.at[0], near)

    def to_far(src):
        return rc(src, far_slot, cy_s.at[1], cy_r.at[1], far)

    def spread_own(outer):
        kind = 0 if outer else 1
        xs_full(kind, 0).start()
        xs_full(kind, 1).start()
        to_core(kind, 0).start()

    def relay(kind):
        for d in range(2):
            from_full(kind, d).wait_recv()
            xs_half(kind, d).start()
        to_core(kind, 1).start()
        to_core(kind, 2).start()

    def relayed(kind):
        for d in range(2):
            sent.append((xs_half, (kind, d)))
            sent.append((to_core, (kind, 1 + d)))

    def finish(kind):
        for d in range(2):
            from_half(kind, d).wait_recv()
        go(to_core, kind, 3)

    def when_outer(run):
        pl.when(middle == 0)(run)

    def when_middle(run):
        pl.when(middle == 1)(run)

    ld_cot.wait()
    go(to_near)
    when_middle(lambda: to_far(mine).start())
    when_outer(lambda: spread_own(True))
    when_middle(lambda: spread_own(False))

    hrows = tok // HCH

    def hpiece(ref, i):
        return ref.at[pl.ds(i * hrows, hrows)]

    def h_first(i):
        return rc(hpiece(hid.at[0], i), hpiece(hrel, i), h_s.at[0, i], h_r.at[0, i], first)

    def h_second(i):
        return rc(hpiece(hrel, i), hpiece(hid.at[1], i), h_s.at[1, i], h_r.at[1, i], second)

    def hrelay(i):
        h_first(i).wait_recv()
        go(h_second, i)

    ld_hid.wait()
    go(h_first, 0)
    go(h_first, 1)

    def out_part(t, cc):
        yp = lax.rem(y_lo + 1 + lax.rem(t, 2), 2)
        g = (yp * NX + lax.rem(x + zigzag(t // 2, 2), NX)) * 2 + cc
        wg = w[pl.ds(pl.multiple_of(g * feat, feat), feat), :]
        return lax.dot_general(hid[0], wg, (((1,), (1,)), ((), ())), preferred_element_type=F32)

    def o_copy(t):
        return rc(o_send.at[t], o_sum.at[t], o_s.at[t], o_r.at[t], core)

    def send_out(t, _):
        o_send[t] = out_part(t, 1 - c)
        o_copy(t).start()
        return 0

    def add_out(t, _):
        o_copy(t).wait_recv()
        o_sum[t] = o_sum[t] + out_part(t, c)
        return 0

    for copy in ld_w:
        copy.wait()
    lax.fori_loop(0, 8, send_out, 0)

    from_near().wait_recv()

    def outer_near():
        to_far(near_slot).start()
        spread_own(False)
        relay(0)

    def middle_near():
        spread_own(True)
        to_far(far_slot).wait_recv()
        xs_full(2, 0).start()
        xs_full(2, 1).start()
        to_core(2, 0).start()

    when_outer(outer_near)
    when_middle(middle_near)
    for kind in range(3):
        sent.extend([(xs_full, (kind, 0)), (xs_full, (kind, 1)), (to_core, (kind, 0))])
        relayed(kind)

    hrelay(0)
    go(h_first, 2)
    lax.fori_loop(0, 2, add_out, 0)
    hrelay(1)
    go(h_first, 3)

    def outer_far():
        to_far(far_slot).wait_recv()
        xs_full(2, 0).start()
        xs_full(2, 1).start()
        to_core(2, 0).start()

    when_outer(outer_far)
    when_middle(lambda: relay(0))
    lax.fori_loop(2, 6, add_out, 0)
    hrelay(2)
    relay(2)
    lax.fori_loop(6, 8, add_out, 0)
    finish(0)
    hrelay(3)
    relay(1)

    def xo_half(d, q):
        src = o_sum.at[q].at[pl.ds(d * half, half)]
        return rc(src, xh.at[d, q], xo_s.at[0, d, q], xo_r.at[0, d, q], x_dev[d])

    def xo_full(d, q):
        return rc(o_sum.at[2 + 2 * d + q], xf.at[d, q], xo_s.at[1, d, q], xo_r.at[1, d, q], x_dev[d])

    for q in range(2):
        for d in range(2):
            go(xo_half, d, q)
    finish(2)
    for kind in (0, 2):
        for j in range(4):
            from_core(kind, j).wait_recv()
    for i in range(HCH):
        h_second(i).wait_recv()

    def w_part(i, _):
        zz = lax.rem(z + zigzag(i, 4), NZ)
        dims = (((0,), (0,)), ((), ()))
        part[i] = lax.dot_general(
            cot[y_hi * NZ + zz], hid[0], dims, preferred_element_type=F32
        ) + lax.dot_general(cot[16 + zz], hid[1], dims, preferred_element_type=F32)
        return 0

    index_of = {4: 0, 3: 1, 5: 2, 2: 3, 6: 4, 1: 5, 7: 6, 0: 7}

    def z_rows(d, m):
        k = 4 - (m + 1) // 2
        return index_of[(k if d == 0 else -k) % NZ], ((m + d) % 2) * rows

    def z_copy(d, m):
        src = zs.at[d, m] if m < 2 else zb.at[d, m - 2]
        return rc(src, zb.at[d, m], z_s.at[d, m], z_r.at[d, m], z_dev[d])

    def coded(v):
        high = v.astype(BF16)
        near_v = high.astype(F32)
        fit = jnp.abs(near_v) > 1e-36
        ratio = jnp.where(fit, (v - near_v) / jnp.where(fit, near_v, 1.0), 0.0)
        return high, jnp.clip(jnp.round(ratio * 2560.0), -10.0, 10.0)

    def take(ref, r):
        low = ref[pl.ds(rows + r, ZR)].astype(F32)
        q0 = jnp.round(low * (1.0 / 21.0))
        q1 = low - 21.0 * q0
        h0 = ref[pl.ds(r, ZR)].astype(F32)
        h1 = ref[pl.ds(rows // 2 + r, ZR)].astype(F32)
        return h0 + h0 * (q0 * (1.0 / 2560.0)), h1 + h1 * (q1 * (1.0 / 2560.0))

    def put(ref, r, v0, v1):
        h0, q0 = coded(v0)
        h1, q1 = coded(v1)
        ref[pl.ds(r, ZR)] = h0
        ref[pl.ds(rows // 2 + r, ZR)] = h1
        ref[pl.ds(rows + r, ZR)] = (q0 * 21.0 + q1).astype(BF16)

    def in_rows(run):
        def body(i, _):
            run(pl.multiple_of(i * ZR, ZR))
            return 0

        lax.fori_loop(0, rows // 2 // ZR, body, 0)

    def part_rows(i, start, r):
        at = pl.ds(start + r, ZR), pl.ds(start + rows // 2 + r, ZR)
        return part[i, at[0]], part[i, at[1]]

    def z_first(d, m):
        i, start = z_rows(d, m)

        def run(r):
            put(zs.at[d, m], r, *part_rows(i, start, r))

        in_rows(run)
        go(z_copy, d, m)

    def z_one(d, m):
        z_copy(d, m - 2).wait_recv()
        i, start = z_rows(d, m)

        def run(r):
            p0, p1 = part_rows(i, start, r)
            s0, s1 = take(zb.at[d, m - 2], r)
            put(zb.at[d, m - 2], r, s0 + p0, s1 + p1)

        in_rows(run)
        go(z_copy, d, m)

    def z_step(m):
        z_one(0, m)
        z_one(1, m)

    lax.fori_loop(0, 1, w_part, 0)
    z_first(0, 0)
    z_first(1, 0)
    lax.fori_loop(1, 3, w_part, 0)
    z_first(0, 1)
    z_first(1, 1)
    lax.fori_loop(3, 8, w_part, 0)
    finish(1)
    for j in range(4):
        from_core(1, j).wait_recv()

    def h_part(g, _):
        acc[...] = acc[...] + jnp.dot(
            cot[g], w[pl.ds(pl.multiple_of(g * feat, feat), feat), :], preferred_element_type=F32
        )
        return 0

    acc[...] = jnp.dot(cot[0], w[pl.ds(0, feat), :], preferred_element_type=F32)
    lax.fori_loop(1, 16, h_part, 0)
    hgb[...] = acc[...].astype(BF16)
    st_hg = pltpu.make_async_copy(hgb, hidden_grad, store_sem.at[0])
    st_hg.start()

    def xo_add(q):
        xo_half(0, q).wait_recv()
        o_sum[2 + q, pl.ds(0, half)] = o_sum[2 + q, pl.ds(0, half)] + xh[0, q]
        go(xo_full, 0, q)
        xo_half(1, q).wait_recv()
        o_sum[4 + q, pl.ds(half, half)] = o_sum[4 + q, pl.ds(half, half)] + xh[1, q]
        go(xo_full, 1, q)

    def xo_end(q):
        for d in range(2):
            xo_full(d, q).wait_recv()
        o_sum[6 + q] = o_sum[6 + q] + xf[0, q] + xf[1, q]

    def yo():
        return rc(o_sum.at[6], yb, yo_s.at[0], yo_r.at[0], near)

    z_step(2)
    xo_add(0)
    xo_add(1)
    z_step(3)
    z_step(4)
    xo_end(0)
    go(yo)
    z_step(5)
    xo_end(1)
    z_step(6)
    yo().wait_recv()
    outb[...] = (o_sum[7] + yb[...]).astype(BF16)
    st_out = pltpu.make_async_copy(outb, output, store_sem.at[1])
    st_out.start()

    def z_end(start, m0, m1):
        z_copy(0, m0).wait_recv()
        z_copy(1, m1).wait_recv()

        def run(r):
            p0, p1 = part_rows(7, start, r)
            s0, s1 = take(zb.at[0, m0], r)
            t0, t1 = take(zb.at[1, m1], r)
            part[7, pl.ds(start + r, ZR)] = (p0 + s0 + t0) * scale
            part[7, pl.ds(start + rows // 2 + r, ZR)] = (p1 + s1 + t1) * scale

        in_rows(run)

    z_end(0, 6, 5)
    z_end(rows, 5, 6)
    st_wg = pltpu.make_async_copy(part.at[7], weight_grad, store_sem.at[2])
    st_wg.start()

    to_far(mine).wait_send()

    def sent_out(t, _):
        o_copy(t).wait_send()
        return 0

    lax.fori_loop(0, 8, sent_out, 0)
    for make, where in sent:
        make(*where).wait_send()
    st_hg.wait()
    st_out.wait()
    st_wg.wait()


def shards(hidden, weight, cotangent):
    tok, ff = hidden.shape
    d_all = weight.shape[0]
    feat = cotangent.shape[1]
    scale = float(tok * lax.axis_size("gx")) ** (-0.5)
    any_space = pl.BlockSpec(memory_space=pl.ANY)
    sem = pltpu.SemaphoreType.DMA
    v = pltpu.VMEM
    return pl.pallas_call(
        functools.partial(kernel, scale),
        out_shape=(
            jax.ShapeDtypeStruct((tok, feat), BF16),
            jax.ShapeDtypeStruct((tok, ff), BF16),
            jax.ShapeDtypeStruct((feat, ff), F32),
        ),
        in_specs=[any_space] * 3,
        out_specs=(any_space,) * 3,
        scratch_shapes=[
            v((d_all, ff), BF16),
            v((2, tok, ff), BF16),
            v((tok, ff), BF16),
            v((24, tok, feat), BF16),
            v((8, tok, feat), F32),
            v((8, tok, feat), F32),
            v((2, 2, tok // 2, feat), F32),
            v((2, 2, tok, feat), F32),
            v((tok, feat), F32),
            v((8, feat, ff), F32),
            v((2, 2, feat * 3 // 4, ff), BF16),
            v((2, 7, feat * 3 // 4, ff), BF16),
            v((tok, ff), F32),
            v((tok, ff), BF16),
            v((tok, feat), BF16),
            sem((2 + WCH,)),
            sem((3,)),
            sem((2,)),
            sem((2,)),
            sem((3, 4)),
            sem((3, 4)),
            sem((3, 4)),
            sem((3, 4)),
            sem((2, HCH)),
            sem((2, HCH)),
            sem((8,)),
            sem((8,)),
            sem((2, 2, 2)),
            sem((2, 2, 2)),
            sem((1,)),
            sem((1,)),
            sem((2, 7)),
            sem((2, 7)),
        ],
        compiler_params=pltpu.CompilerParams(
            collective_id=0, has_side_effects=True, vmem_limit_bytes=62 * 1024 * 1024
        ),
    )(hidden, weight, cotangent)


def solution(mesh):
    placed = (P("gx", "gy"), P(None, "gy"), P("gx", "gy"))
    return jax.shard_map(
        shards,
        mesh=mesh,
        in_specs=placed,
        out_specs=(P("gx", "gy"), P("gx", "gy"), P("gx", "gy")),
        check_vma=False,
    )
```

```python
import functools

import jax
import jax.numpy as jnp
from jax import lax
from jax.experimental import pallas as pl
from jax.experimental.pallas import tpu as pltpu
from jax.sharding import PartitionSpec as P

MESH = pl.DeviceIdType.MESH
F32 = jnp.float32
BF16 = jnp.bfloat16
NX, NZ = 4, 8
HCH = 2
GROUPS = ((0, 512), (512, 384))
WCH = 4
ZR = 16


def zigzag(i, top):
    odd = lax.rem(i, 2)
    return top + (1 - odd) * (i // 2) - odd * ((i + 1) // 2)


def kernel(
    scale,
    hidden,
    weight,
    cotangent,
    output,
    hidden_grad,
    weight_grad,
    w,
    hid,
    hrel,
    cot,
    o_send,
    o_sum,
    xh,
    xf,
    yb,
    part,
    zs0,
    zs1,
    zb0,
    zb1,
    acc,
    load_sem,
    cy_s,
    cy_r,
    cx_s,
    cx_r,
    cd_s,
    cd_r,
    h_s,
    h_r,
    o_s,
    o_r,
    xo_s,
    xo_r,
    yo_s,
    yo_r,
    z_s,
    z_r,
):
    gx = lax.axis_index("gx")
    gy = lax.axis_index("gy")
    y_hi, z = gx // NZ, lax.rem(gx, NZ)
    c = lax.rem(gy, 2)
    x = lax.rem(gy // 2, NX)
    y_lo = gy // (2 * NX)
    tok, ff = hid.shape[1], hid.shape[2]
    feat = cot.shape[2]
    half = tok // 2
    rows = feat // 2

    def dev(yh, yl, xx, zz, cc):
        return (yh * NZ + zz, (yl * NX + xx) * 2 + cc)

    right, left = lax.rem(x + 1, NX), lax.rem(x + NX - 1, NX)
    across = lax.rem(x + 2, NX)
    core = dev(y_hi, y_lo, x, z, 1 - c)
    near = dev(y_hi, 1 - y_lo, x, z, c)
    far = dev(1 - y_hi, 1 - y_lo, x, z, c)
    first = dev(lax.rem(y_hi + c, 2), 1 - y_lo, x, z, c)
    second = dev(lax.rem(y_hi + 1 - c, 2), 1 - y_lo, x, z, c)
    x_dev = (dev(y_hi, y_lo, right, z, c), dev(y_hi, y_lo, left, z, c))
    z_dev = (
        dev(y_hi, y_lo, x, lax.rem(z + 1, NZ), c),
        dev(y_hi, y_lo, x, lax.rem(z + NZ - 1, NZ), c),
    )

    def rc(src, dst, ss, rs, to):
        return pltpu.make_async_remote_copy(
            src_ref=src, dst_ref=dst, send_sem=ss, recv_sem=rs, device_id=to, device_id_type=MESH
        )

    sent = []

    def go(make, *where):
        make(*where).start()
        sent.append((make, where))

    base = (y_hi * NX * 2, (1 - y_hi) * NX * 2, 16)
    middle = lax.rem(y_hi + y_lo, 2)

    def slot(kind, xx):
        return cot.at[base[kind] + xx * 2 + c]

    mine = cot.at[y_lo * NX * 2 + x * 2 + c]
    near_slot = cot.at[(1 - y_lo) * NX * 2 + x * 2 + c]
    far_slot = slot(2, x)
    ld_cot = pltpu.make_async_copy(cotangent, mine, load_sem.at[0])
    ld_hid = pltpu.make_async_copy(hidden, hid.at[0], load_sem.at[1])
    ld_cot.start()
    ld_hid.start()
    wrows = w.shape[0] // WCH
    ld_w = [
        pltpu.make_async_copy(
            weight.at[pl.ds(i * wrows, wrows)], w.at[pl.ds(i * wrows, wrows)], load_sem.at[2 + i]
        )
        for i in range(WCH)
    ]
    for copy in ld_w:
        copy.start()

    barrier = pltpu.get_barrier_semaphore()
    peers = (core, near, far, *x_dev, *z_dev)
    for peer in peers:
        pl.semaphore_signal(barrier, inc=1, device_id=peer, device_id_type=MESH)
    pl.semaphore_wait(barrier, len(peers))

    def half_of(ref, h):
        return ref.at[pl.ds(h * half, half)]

    def xs_full(kind, d, h):
        ref = half_of(slot(kind, x), h)
        return rc(ref, ref, cx_s.at[kind, d, h], cx_r.at[kind, d, h], x_dev[d])

    def xs_relay(kind, d):
        ref = half_of(slot(kind, (left, right)[d]), d)
        return rc(ref, ref, cx_s.at[kind, d, 2], cx_r.at[kind, d, 2], x_dev[d])

    def from_full(kind, d, h):
        ref = half_of(slot(kind, (left, right)[d]), h)
        return rc(ref, ref, cx_s.at[kind, d, h], cx_r.at[kind, d, h], x_dev[d])

    def from_relay(kind, d):
        ref = half_of(slot(kind, across), d)
        return rc(ref, ref, cx_s.at[kind, d, 2], cx_r.at[kind, d, 2], x_dev[d])

    def to_core(kind, j):
        ref = slot(kind, (x, left, right, across)[j])
        return rc(ref, ref, cd_s.at[kind, j], cd_r.at[kind, j], core)

    def from_core(kind, j):
        ref = cot.at[base[kind] + (x, left, right, across)[j] * 2 + 1 - c]
        return rc(ref, ref, cd_s.at[kind, j], cd_r.at[kind, j], core)

    def to_near(h):
        ref = half_of(mine, h)
        return rc(ref, ref, cy_s.at[0, h], cy_r.at[0, h], near)

    def from_near(h):
        ref = half_of(near_slot, h)
        return rc(ref, ref, cy_s.at[0, h], cy_r.at[0, h], near)

    def to_far(src, h):
        return rc(half_of(src, h), half_of(far_slot, h), cy_s.at[1, h], cy_r.at[1, h], far)

    def spread(kind, h):
        xs_full(kind, 0, h).start()
        xs_full(kind, 1, h).start()

    def relay(kind):
        for d in range(2):
            from_full(kind, d, d).wait_recv()
            xs_relay(kind, d).start()
        for d in range(2):
            from_full(kind, d, 1 - d).wait_recv()
            to_core(kind, 1 + d).start()

    def finish(kind):
        for d in range(2):
            from_relay(kind, d).wait_recv()
        to_core(kind, 3).start()

    outer, inner = pl.when(middle == 0), pl.when(middle == 1)

    ld_cot.wait()

    @outer
    def _():
        for h in range(2):
            to_near(h).start()
            spread(0, h)
        to_core(0, 0).start()

    @inner
    def _():
        for h in range(2):
            to_near(h).start()
            to_far(mine, h).start()
        spread(1, 0)
        to_core(1, 0).start()

    hrows = tok // HCH

    def hpiece(ref, g, i):
        return ref.at[pl.ds(i * hrows, hrows), pl.ds(*GROUPS[g])]

    def h_first(g, i):
        at = g, i
        return rc(hpiece(hid.at[0], g, i), hpiece(hrel, g, i), h_s.at[0, *at], h_r.at[0, *at], first)

    def h_second(g, i):
        at = g, i
        return rc(hpiece(hrel, g, i), hpiece(hid.at[1], g, i), h_s.at[1, *at], h_r.at[1, *at], second)

    def hrelay(g, i):
        h_first(g, i).wait_recv()
        go(h_second, g, i)

    ld_hid.wait()
    for i in range(HCH):
        go(h_first, 0, i)

    def out_part(t, cc):
        yp = lax.rem(y_lo + 1 + lax.rem(t, 2), 2)
        g = (yp * NX + lax.rem(x + zigzag(t // 2, 2), NX)) * 2 + cc
        wg = w[pl.ds(pl.multiple_of(g * feat, feat), feat), :]
        return lax.dot_general(hid[0], wg, (((1,), (1,)), ((), ())), preferred_element_type=F32)

    def o_copy(t):
        return rc(o_send.at[t], o_sum.at[t], o_s.at[t], o_r.at[t], core)

    def send_out(t, _):
        o_send[t] = out_part(t, 1 - c)
        o_copy(t).start()
        return 0

    def add_out(t, _):
        o_copy(t).wait_recv()
        o_sum[t] = o_sum[t] + out_part(t, c)
        return 0

    for copy in ld_w:
        copy.wait()
    lax.fori_loop(0, 6, send_out, 0)

    @outer
    def _():
        for h in range(2):
            from_near(h).wait_recv()
            to_far(near_slot, h).start()
        to_core(1, 0).start()
        relay(0)

    @inner
    def _():
        for h in range(2):
            from_near(h).wait_recv()
            spread(0, h)
            to_far(far_slot, h).wait_recv()
            spread(2, h)
        spread(1, 1)
        to_core(0, 0).start()
        to_core(2, 0).start()

    lax.fori_loop(6, 8, send_out, 0)
    hrelay(0, 0)

    @outer
    def _():
        for h in range(2):
            to_far(far_slot, h).wait_recv()
            spread(2, h)
        for h in range(2):
            spread(1, h)
        to_core(2, 0).start()

    hrelay(0, 1)
    for i in range(HCH):
        go(h_first, 1, i)
    lax.fori_loop(0, 2, add_out, 0)
    inner(lambda: relay(0))
    lax.fori_loop(2, 4, add_out, 0)
    relay(2)
    finish(0)
    hrelay(1, 0)
    lax.fori_loop(4, 6, add_out, 0)
    hrelay(1, 1)
    finish(2)
    relay(1)
    lax.fori_loop(6, 8, add_out, 0)

    def xo_half(d, q):
        src = o_sum.at[q].at[pl.ds(d * half, half)]
        return rc(src, xh.at[d, q], xo_s.at[0, d, q], xo_r.at[0, d, q], x_dev[d])

    def xo_full(d, q):
        return rc(o_sum.at[2 + 2 * d + q], xf.at[d, q], xo_s.at[1, d, q], xo_r.at[1, d, q], x_dev[d])

    for q in range(2):
        for d in range(2):
            go(xo_half, d, q)
    for kind in (0, 2):
        for j in range(4):
            from_core(kind, j).wait_recv()

    def w_part(g):
        def body(i, _):
            zz = lax.rem(z + zigzag(i, 4), NZ)
            dims = (((0,), (0,)), ((), ()))
            cols = pl.ds(*GROUPS[g])
            part[i, :, cols] = lax.dot_general(
                cot[y_hi * NZ + zz], hid[0, :, cols], dims, preferred_element_type=F32
            ) + lax.dot_general(cot[16 + zz], hid[1, :, cols], dims, preferred_element_type=F32)
            return 0

        return body

    index_of = {4: 0, 3: 1, 5: 2, 2: 3, 6: 4, 1: 5, 7: 6, 0: 7}

    zs, zb = (zs0, zs1), (zb0, zb1)
    quarter = rows // 4

    def z_rows(d, m):
        k = 4 - (m + 1) // 2
        return index_of[(k if d == 0 else -k) % NZ], ((m + d) % 2) * rows

    def z_copy(d, m, g):
        src = zs[g].at[d, m] if m < 2 else zb[g].at[d, m - 2]
        return rc(src, zb[g].at[d, m], z_s.at[g, d, m], z_r.at[g, d, m], z_dev[d])

    def coded(v):
        high = v.astype(BF16)
        near_v = high.astype(F32)
        fit = jnp.abs(near_v) > 1e-36
        ratio = jnp.where(fit, (v - near_v) / jnp.where(fit, near_v, 1.0), 0.0)
        return high, jnp.clip(jnp.round(ratio * 1792.0), -7.0, 7.0)

    def parted(p):
        q = jnp.round(p * (1.0 / 15.0))
        return q, p - 15.0 * q

    def take(ref, r):
        low = ref[pl.ds(rows + r, ZR)].astype(F32)
        size = jnp.abs(low)
        e = jnp.floor(jnp.log2(size) + 1.0 / 512.0)
        f = jnp.round((size * jnp.exp2(-e) - 1.0) * 128.0)
        codes = (*parted(e), *parted(jnp.where(low < 0.0, -f, f)))
        high = [ref[pl.ds(j * quarter + r, ZR)].astype(F32) for j in range(4)]
        return [h + h * (q * (1.0 / 1792.0)) for h, q in zip(high, codes)]

    def put(ref, r, values):
        q = []
        for j, v in enumerate(values):
            high, code = coded(v)
            ref[pl.ds(j * quarter + r, ZR)] = high
            q.append(code)
        e, f = q[0] * 15.0 + q[1], q[2] * 15.0 + q[3]
        size = jnp.exp2(e) * (1.0 + jnp.abs(f) * (1.0 / 128.0))
        ref[pl.ds(rows + r, ZR)] = jnp.where(f < 0.0, -size, size).astype(BF16)

    def in_rows(run):
        def body(i, _):
            run(pl.multiple_of(i * ZR, ZR))
            return 0

        lax.fori_loop(0, quarter // ZR, body, 0)

    def part_rows(i, start, r, g):
        return [part[i, pl.ds(start + j * quarter + r, ZR), pl.ds(*GROUPS[g])] for j in range(4)]

    def z_first(d, m, g):
        i, start = z_rows(d, m)
        in_rows(lambda r: put(zs[g].at[d, m], r, part_rows(i, start, r, g)))
        go(z_copy, d, m, g)

    def z_one(d, m, g):
        z_copy(d, m - 2, g).wait_recv()
        i, start = z_rows(d, m)
        ref = zb[g].at[d, m - 2]

        def run(r):
            own = part_rows(i, start, r, g)
            put(ref, r, [s + p for s, p in zip(take(ref, r), own)])

        in_rows(run)
        go(z_copy, d, m, g)

    def z_step(m):
        for g in range(2):
            z_one(0, m, g)
            z_one(1, m, g)

    def z_start(g):
        for i in range(HCH):
            h_second(g, i).wait_recv()
        run = w_part(g)
        lax.fori_loop(0, 1, run, 0)
        z_first(0, 0, g)
        z_first(1, 0, g)
        lax.fori_loop(1, 3, run, 0)
        z_first(0, 1, g)
        z_first(1, 1, g)

    z_start(0)
    z_start(1)
    lax.fori_loop(3, 8, w_part(0), 0)
    lax.fori_loop(3, 8, w_part(1), 0)
    finish(1)
    for j in range(4):
        from_core(1, j).wait_recv()

    def h_part(g, _):
        acc[...] = acc[...] + jnp.dot(
            cot[g], w[pl.ds(pl.multiple_of(g * feat, feat), feat), :], preferred_element_type=F32
        )
        return 0

    def xo_add(q):
        xo_half(0, q).wait_recv()
        o_sum[2 + q, pl.ds(0, half)] = o_sum[2 + q, pl.ds(0, half)] + xh[0, q]
        go(xo_full, 0, q)
        xo_half(1, q).wait_recv()
        o_sum[4 + q, pl.ds(half, half)] = o_sum[4 + q, pl.ds(half, half)] + xh[1, q]
        go(xo_full, 1, q)

    def xo_end(q):
        for d in range(2):
            xo_full(d, q).wait_recv()
        o_sum[6 + q] = o_sum[6 + q] + xf[0, q] + xf[1, q]

    def yo():
        return rc(o_sum.at[6], yb, yo_s.at[0], yo_r.at[0], near)

    xo_add(0)
    xo_add(1)
    acc[...] = jnp.dot(cot[0], w[pl.ds(0, feat), :], preferred_element_type=F32)
    lax.fori_loop(1, 8, h_part, 0)
    z_step(2)
    lax.fori_loop(8, 16, h_part, 0)
    hidden_grad[...] = acc[...].astype(BF16)
    z_step(3)
    z_step(4)
    xo_end(0)
    go(yo)
    z_step(5)
    xo_end(1)
    z_step(6)
    yo().wait_recv()
    output[...] = (o_sum[7] + yb[...]).astype(BF16)

    def z_end(start, m0, m1, g):
        z_copy(0, m0, g).wait_recv()
        z_copy(1, m1, g).wait_recv()

        def run(r):
            own = part_rows(7, start, r, g)
            sums = zip(own, take(zb[g].at[0, m0], r), take(zb[g].at[1, m1], r))
            for j, (p, s, t) in enumerate(sums):
                weight_grad[pl.ds(start + j * quarter + r, ZR), pl.ds(*GROUPS[g])] = (p + s + t) * scale

        in_rows(run)

    for h in range(2):
        to_near(h).wait_send()
        to_far(mine, h).wait_send()
    for kind in range(3):
        for d in range(2):
            for h in range(2):
                xs_full(kind, d, h).wait_send()
            xs_relay(kind, d).wait_send()
        for j in range(4):
            to_core(kind, j).wait_send()

    def sent_out(t, _):
        o_copy(t).wait_send()
        return 0

    lax.fori_loop(0, 8, sent_out, 0)
    for g in range(2):
        z_end(0, 6, 5, g)
        z_end(rows, 5, 6, g)
    for make, where in sent:
        make(*where).wait_send()


def store(a, b, d, a_out, b_out, d_out, sems):
    pairs = ((a, a_out), (b, b_out), (d, d_out))
    copies = [pltpu.make_async_copy(s, t, sems.at[i]) for i, (s, t) in enumerate(pairs)]
    for copy in copies:
        copy.start()
    for copy in copies:
        copy.wait()


def shards(hidden, weight, cotangent):
    tok, ff = hidden.shape
    d_all = weight.shape[0]
    feat = cotangent.shape[1]
    scale = float(tok * lax.axis_size("gx")) ** (-0.5)
    any_space = pl.BlockSpec(memory_space=pl.ANY)
    vmem_space = pl.BlockSpec(memory_space=pltpu.VMEM)
    sem = pltpu.SemaphoreType.DMA
    v = pltpu.VMEM
    shapes = (((tok, feat), BF16), ((tok, ff), BF16), ((feat, ff), F32))
    args = [pltpu.with_memory_space_constraint(a, pltpu.HBM) for a in (hidden, weight, cotangent)]
    results = pl.pallas_call(
        functools.partial(kernel, scale),
        out_shape=tuple(v(*shape) for shape in shapes),
        in_specs=[any_space] * 3,
        out_specs=(vmem_space,) * 3,
        scratch_shapes=[
            v((d_all, ff), BF16),
            v((2, tok, ff), BF16),
            v((tok, ff), BF16),
            v((24, tok, feat), BF16),
            v((8, tok, feat), F32),
            v((8, tok, feat), F32),
            v((2, 2, tok // 2, feat), F32),
            v((2, 2, tok, feat), F32),
            v((tok, feat), F32),
            v((8, feat, ff), F32),
            *(v((2, n, feat * 5 // 8, size), BF16) for n in (2, 7) for _, size in GROUPS),
            v((tok, ff), F32),
            sem((2 + WCH,)),
            sem((2, 2)),
            sem((2, 2)),
            sem((3, 2, 3)),
            sem((3, 2, 3)),
            sem((3, 4)),
            sem((3, 4)),
            sem((2, 2, HCH)),
            sem((2, 2, HCH)),
            sem((8,)),
            sem((8,)),
            sem((2, 2, 2)),
            sem((2, 2, 2)),
            sem((1,)),
            sem((1,)),
            sem((2, 2, 7)),
            sem((2, 2, 7)),
        ],
        compiler_params=pltpu.CompilerParams(
            collective_id=0, has_side_effects=True, vmem_limit_bytes=50 * 1024 * 1024
        ),
    )(*args)
    return pl.pallas_call(
        store,
        out_shape=tuple(jax.ShapeDtypeStruct(*shape) for shape in shapes),
        in_specs=[any_space] * 3,
        out_specs=(pl.BlockSpec(memory_space=pltpu.HBM),) * 3,
        scratch_shapes=[sem((3,))],
        compiler_params=pltpu.CompilerParams(vmem_limit_bytes=1024 * 1024),
    )(*results)


def solution(mesh):
    placed = (P("gx", "gy"), P(None, "gy"), P("gx", "gy"))
    return jax.shard_map(
        shards,
        mesh=mesh,
        in_specs=placed,
        out_specs=(P("gx", "gy"), P("gx", "gy"), P("gx", "gy")),
        check_vma=False,
    )
```

```python
import functools

import jax
import jax.numpy as jnp
from jax import lax
from jax.experimental import pallas as pl
from jax.experimental.pallas import tpu as pltpu
from jax.sharding import PartitionSpec as P

MESH = pl.DeviceIdType.MESH
F32 = jnp.float32
BF16 = jnp.bfloat16
NX, NZ = 4, 8
HCH = 2
GROUPS = ((0, 512), (512, 384))
WCH = 4
ZR = 16


def zigzag(i, top):
    odd = lax.rem(i, 2)
    return top + (1 - odd) * (i // 2) - odd * ((i + 1) // 2)


def kernel(
    scale,
    hidden,
    weight,
    cotangent,
    output,
    hidden_grad,
    weight_grad,
    w,
    hid,
    hrel,
    cot,
    o_send,
    o_sum,
    xh,
    xf,
    yb,
    part,
    zs0,
    zs1,
    zb0,
    zb1,
    acc,
    hgb,
    outb,
    load_sem,
    store_sem,
    cy_s,
    cy_r,
    cx_s,
    cx_r,
    cd_s,
    cd_r,
    h_s,
    h_r,
    o_s,
    o_r,
    xo_s,
    xo_r,
    yo_s,
    yo_r,
    z_s,
    z_r,
):
    gx = lax.axis_index("gx")
    gy = lax.axis_index("gy")
    y_hi, z = gx // NZ, lax.rem(gx, NZ)
    c = lax.rem(gy, 2)
    x = lax.rem(gy // 2, NX)
    y_lo = gy // (2 * NX)
    tok, ff = hid.shape[1], hid.shape[2]
    feat = cot.shape[2]
    half = tok // 2
    rows = feat // 2

    def dev(yh, yl, xx, zz, cc):
        return (yh * NZ + zz, (yl * NX + xx) * 2 + cc)

    right, left = lax.rem(x + 1, NX), lax.rem(x + NX - 1, NX)
    across = lax.rem(x + 2, NX)
    core = dev(y_hi, y_lo, x, z, 1 - c)
    near = dev(y_hi, 1 - y_lo, x, z, c)
    far = dev(1 - y_hi, 1 - y_lo, x, z, c)
    first = dev(lax.rem(y_hi + c, 2), 1 - y_lo, x, z, c)
    second = dev(lax.rem(y_hi + 1 - c, 2), 1 - y_lo, x, z, c)
    x_dev = (dev(y_hi, y_lo, right, z, c), dev(y_hi, y_lo, left, z, c))
    z_dev = (
        dev(y_hi, y_lo, x, lax.rem(z + 1, NZ), c),
        dev(y_hi, y_lo, x, lax.rem(z + NZ - 1, NZ), c),
    )

    def rc(src, dst, ss, rs, to):
        return pltpu.make_async_remote_copy(
            src_ref=src, dst_ref=dst, send_sem=ss, recv_sem=rs, device_id=to, device_id_type=MESH
        )

    sent = []

    def go(make, *where):
        make(*where).start()
        sent.append((make, where))

    base = (y_hi * NX * 2, (1 - y_hi) * NX * 2, 16)
    middle = lax.rem(y_hi + y_lo, 2)

    def slot(kind, xx):
        return cot.at[base[kind] + xx * 2 + c]

    mine = cot.at[y_lo * NX * 2 + x * 2 + c]
    near_slot = cot.at[(1 - y_lo) * NX * 2 + x * 2 + c]
    far_slot = slot(2, x)
    ld_cot = pltpu.make_async_copy(cotangent, mine, load_sem.at[0])
    ld_hid = pltpu.make_async_copy(hidden, hid.at[0], load_sem.at[1])
    ld_cot.start()
    ld_hid.start()
    wrows = w.shape[0] // WCH
    ld_w = [
        pltpu.make_async_copy(
            weight.at[pl.ds(i * wrows, wrows)], w.at[pl.ds(i * wrows, wrows)], load_sem.at[2 + i]
        )
        for i in range(WCH)
    ]
    for copy in ld_w:
        copy.start()

    barrier = pltpu.get_barrier_semaphore()
    peers = (core, near, far, *x_dev, *z_dev)
    for peer in peers:
        pl.semaphore_signal(barrier, inc=1, device_id=peer, device_id_type=MESH)
    pl.semaphore_wait(barrier, len(peers))

    def half_of(ref, h):
        return ref.at[pl.ds(h * half, half)]

    def xs_full(kind, d, h):
        ref = half_of(slot(kind, x), h)
        return rc(ref, ref, cx_s.at[kind, d, h], cx_r.at[kind, d, h], x_dev[d])

    def xs_relay(kind, d):
        ref = half_of(slot(kind, (left, right)[d]), d)
        return rc(ref, ref, cx_s.at[kind, d, 2], cx_r.at[kind, d, 2], x_dev[d])

    def from_full(kind, d, h):
        ref = half_of(slot(kind, (left, right)[d]), h)
        return rc(ref, ref, cx_s.at[kind, d, h], cx_r.at[kind, d, h], x_dev[d])

    def from_relay(kind, d):
        ref = half_of(slot(kind, across), d)
        return rc(ref, ref, cx_s.at[kind, d, 2], cx_r.at[kind, d, 2], x_dev[d])

    def to_core(kind, j):
        ref = slot(kind, (x, left, right, across)[j])
        return rc(ref, ref, cd_s.at[kind, j], cd_r.at[kind, j], core)

    def from_core(kind, j):
        ref = cot.at[base[kind] + (x, left, right, across)[j] * 2 + 1 - c]
        return rc(ref, ref, cd_s.at[kind, j], cd_r.at[kind, j], core)

    def to_near(h):
        ref = half_of(mine, h)
        return rc(ref, ref, cy_s.at[0, h], cy_r.at[0, h], near)

    def from_near(h):
        ref = half_of(near_slot, h)
        return rc(ref, ref, cy_s.at[0, h], cy_r.at[0, h], near)

    def to_far(src, h):
        return rc(half_of(src, h), half_of(far_slot, h), cy_s.at[1, h], cy_r.at[1, h], far)

    def spread(kind, h):
        xs_full(kind, 0, h).start()
        xs_full(kind, 1, h).start()

    def relay(kind):
        for d in range(2):
            from_full(kind, d, d).wait_recv()
            xs_relay(kind, d).start()
        for d in range(2):
            from_full(kind, d, 1 - d).wait_recv()
            to_core(kind, 1 + d).start()

    def finish(kind):
        for d in range(2):
            from_relay(kind, d).wait_recv()
        to_core(kind, 3).start()

    outer, inner = pl.when(middle == 0), pl.when(middle == 1)

    ld_cot.wait()

    @outer
    def _():
        for h in range(2):
            to_near(h).start()
            spread(0, h)
        to_core(0, 0).start()

    @inner
    def _():
        for h in range(2):
            to_near(h).start()
            to_far(mine, h).start()
        spread(1, 0)
        to_core(1, 0).start()

    hrows = tok // HCH

    def hpiece(ref, g, i):
        return ref.at[pl.ds(i * hrows, hrows), pl.ds(*GROUPS[g])]

    def h_first(g, i):
        at = g, i
        return rc(hpiece(hid.at[0], g, i), hpiece(hrel, g, i), h_s.at[0, *at], h_r.at[0, *at], first)

    def h_second(g, i):
        at = g, i
        return rc(hpiece(hrel, g, i), hpiece(hid.at[1], g, i), h_s.at[1, *at], h_r.at[1, *at], second)

    def hrelay(g, i):
        h_first(g, i).wait_recv()
        go(h_second, g, i)

    ld_hid.wait()
    for i in range(HCH):
        go(h_first, 0, i)

    def out_part(t, cc):
        yp = lax.rem(y_lo + 1 + lax.rem(t, 2), 2)
        g = (yp * NX + lax.rem(x + zigzag(t // 2, 2), NX)) * 2 + cc
        wg = w[pl.ds(pl.multiple_of(g * feat, feat), feat), :]
        return lax.dot_general(hid[0], wg, (((1,), (1,)), ((), ())), preferred_element_type=F32)

    def o_copy(t):
        return rc(o_send.at[t], o_sum.at[t], o_s.at[t], o_r.at[t], core)

    def send_out(t, _):
        o_send[t] = out_part(t, 1 - c)
        o_copy(t).start()
        return 0

    def add_out(t, _):
        o_copy(t).wait_recv()
        o_sum[t] = o_sum[t] + out_part(t, c)
        return 0

    for copy in ld_w:
        copy.wait()
    lax.fori_loop(0, 6, send_out, 0)

    @outer
    def _():
        for h in range(2):
            from_near(h).wait_recv()
            to_far(near_slot, h).start()
        to_core(1, 0).start()
        relay(0)

    @inner
    def _():
        for h in range(2):
            from_near(h).wait_recv()
            spread(0, h)
            to_far(far_slot, h).wait_recv()
            spread(2, h)
        to_core(0, 0).start()
        to_core(2, 0).start()

    lax.fori_loop(6, 8, send_out, 0)
    hrelay(0, 0)

    @outer
    def _():
        to_far(far_slot, 0).wait_recv()
        spread(2, 0)
        hrelay(0, 1)
        to_far(far_slot, 1).wait_recv()
        spread(2, 1)
        for i in range(HCH):
            h_first(1, i).start()
        to_core(2, 0).start()

    @inner
    def _():
        h_first(0, 1).wait_recv()
        h_second(0, 1).start()
        for i in range(HCH):
            h_first(1, i).start()

    sent.extend((h_first, (1, i)) for i in range(HCH))
    lax.fori_loop(0, 2, add_out, 0)
    inner(lambda: relay(0))
    lax.fori_loop(2, 4, add_out, 0)
    relay(2)
    outer(lambda: spread(1, 0))
    spread(1, 1)
    finish(0)
    hrelay(1, 0)
    lax.fori_loop(4, 6, add_out, 0)
    finish(2)
    hrelay(1, 1)

    def xo_half(d, q):
        src = o_sum.at[q].at[pl.ds(d * half, half)]
        return rc(src, xh.at[d, q], xo_s.at[0, d, q], xo_r.at[0, d, q], x_dev[d])

    def xo_full(d, q):
        return rc(o_sum.at[2 + 2 * d + q], xf.at[d, q], xo_s.at[1, d, q], xo_r.at[1, d, q], x_dev[d])

    def xo_add(q):
        xo_half(0, q).wait_recv()
        o_sum[2 + q, pl.ds(0, half)] = o_sum[2 + q, pl.ds(0, half)] + xh[0, q]
        go(xo_full, 0, q)
        xo_half(1, q).wait_recv()
        o_sum[4 + q, pl.ds(half, half)] = o_sum[4 + q, pl.ds(half, half)] + xh[1, q]
        go(xo_full, 1, q)

    for kind in (0, 2):
        for j in range(4):
            from_core(kind, j).wait_recv()

    def w_part(g):
        def body(i, _):
            zz = lax.rem(z + zigzag(i, 4), NZ)
            dims = (((0,), (0,)), ((), ()))
            cols = pl.ds(*GROUPS[g])
            part[i, :, cols] = lax.dot_general(
                cot[y_hi * NZ + zz], hid[0, :, cols], dims, preferred_element_type=F32
            ) + lax.dot_general(cot[16 + zz], hid[1, :, cols], dims, preferred_element_type=F32)
            return 0

        return body

    index_of = {4: 0, 3: 1, 5: 2, 2: 3, 6: 4, 1: 5, 7: 6, 0: 7}

    zs, zb = (zs0, zs1), (zb0, zb1)
    quarter = rows // 4

    def z_rows(d, m):
        k = 4 - (m + 1) // 2
        return index_of[(k if d == 0 else -k) % NZ], ((m + d) % 2) * rows

    def z_copy(d, m, g):
        src = zs[g].at[d, m] if m < 2 else zb[g].at[d, m - 2]
        return rc(src, zb[g].at[d, m], z_s.at[g, d, m], z_r.at[g, d, m], z_dev[d])

    def coded(v):
        high = v.astype(BF16)
        near_v = high.astype(F32)
        fit = jnp.abs(near_v) > 1e-36
        ratio = jnp.where(fit, (v - near_v) / jnp.where(fit, near_v, 1.0), 0.0)
        return high, jnp.clip(jnp.round(ratio * 1792.0), -7.0, 7.0)

    def parted(p):
        q = jnp.round(p * (1.0 / 15.0))
        return q, p - 15.0 * q

    def take(ref, r):
        low = ref[pl.ds(rows + r, ZR)].astype(F32)
        size = jnp.abs(low)
        e = jnp.floor(jnp.log2(size) + 1.0 / 512.0)
        f = jnp.round((size * jnp.exp2(-e) - 1.0) * 128.0)
        codes = (*parted(e), *parted(jnp.where(low < 0.0, -f, f)))
        high = [ref[pl.ds(j * quarter + r, ZR)].astype(F32) for j in range(4)]
        return [h + h * (q * (1.0 / 1792.0)) for h, q in zip(high, codes)]

    def put(ref, r, values):
        q = []
        for j, v in enumerate(values):
            high, code = coded(v)
            ref[pl.ds(j * quarter + r, ZR)] = high
            q.append(code)
        e, f = q[0] * 15.0 + q[1], q[2] * 15.0 + q[3]
        size = jnp.exp2(e) * (1.0 + jnp.abs(f) * (1.0 / 128.0))
        ref[pl.ds(rows + r, ZR)] = jnp.where(f < 0.0, -size, size).astype(BF16)

    def in_rows(run):
        def body(i, _):
            run(pl.multiple_of(i * ZR, ZR))
            return 0

        lax.fori_loop(0, quarter // ZR, body, 0)

    def part_rows(i, start, r, g):
        return [part[i, pl.ds(start + j * quarter + r, ZR), pl.ds(*GROUPS[g])] for j in range(4)]

    def z_first(d, m, g):
        i, start = z_rows(d, m)
        in_rows(lambda r: put(zs[g].at[d, m], r, part_rows(i, start, r, g)))
        go(z_copy, d, m, g)

    def z_one(d, m, g):
        z_copy(d, m - 2, g).wait_recv()
        i, start = z_rows(d, m)
        ref = zb[g].at[d, m - 2]

        def run(r):
            own = part_rows(i, start, r, g)
            put(ref, r, [s + p for s, p in zip(take(ref, r), own)])

        in_rows(run)
        go(z_copy, d, m, g)

    def z_step(m):
        for g in range(2):
            z_one(0, m, g)
            z_one(1, m, g)

    def z_start(g):
        for i in range(HCH):
            h_second(g, i).wait_recv()
        run = w_part(g)
        lax.fori_loop(0, 1, run, 0)
        z_first(0, 0, g)
        z_first(1, 0, g)
        lax.fori_loop(1, 3, run, 0)
        z_first(0, 1, g)
        z_first(1, 1, g)

    def z_pair(m, g):
        z_one(0, m, g)
        z_one(1, m, g)

    def h_part(g, _):
        acc[...] = acc[...] + jnp.dot(
            cot[g], w[pl.ds(pl.multiple_of(g * feat, feat), feat), :], preferred_element_type=F32
        )
        return 0

    def xo_end(q):
        for d in range(2):
            xo_full(d, q).wait_recv()
        o_sum[6 + q] = o_sum[6 + q] + xf[0, q] + xf[1, q]

    def yo():
        return rc(o_sum.at[6], yb, yo_s.at[0], yo_r.at[0], near)

    z_start(0)
    relay(1)
    for q in range(2):
        for d in range(2):
            go(xo_half, d, q)
    z_start(1)
    lax.fori_loop(6, 8, add_out, 0)
    z_pair(2, 0)
    lax.fori_loop(3, 8, w_part(0), 0)
    z_pair(3, 0)
    xo_add(0)
    z_pair(2, 1)
    lax.fori_loop(3, 8, w_part(1), 0)
    z_pair(3, 1)
    finish(1)
    xo_add(1)
    for j in range(4):
        from_core(1, j).wait_recv()
    z_pair(4, 0)
    acc[...] = jnp.dot(cot[0], w[pl.ds(0, feat), :], preferred_element_type=F32)
    lax.fori_loop(1, 4, h_part, 0)
    z_pair(4, 1)
    lax.fori_loop(4, 9, h_part, 0)
    z_pair(5, 0)
    lax.fori_loop(9, 13, h_part, 0)
    z_pair(5, 1)
    xo_end(0)
    go(yo)
    lax.fori_loop(13, 16, h_part, 0)
    hgb[...] = acc[...].astype(BF16)
    st_hg = pltpu.make_async_copy(hgb, hidden_grad, store_sem.at[0])
    st_hg.start()
    z_pair(6, 0)
    z_pair(6, 1)
    xo_end(1)

    def z_end(start, m0, m1, g):
        z_copy(0, m0, g).wait_recv()
        z_copy(1, m1, g).wait_recv()

        def run(r):
            own = part_rows(7, start, r, g)
            sums = zip(own, take(zb[g].at[0, m0], r), take(zb[g].at[1, m1], r))
            for j, (p, s, t) in enumerate(sums):
                part[7, pl.ds(start + j * quarter + r, ZR), pl.ds(*GROUPS[g])] = (p + s + t) * scale

        in_rows(run)

    def st_wg(g):
        cols = pl.ds(*GROUPS[g])
        return pltpu.make_async_copy(part.at[7, :, cols], weight_grad.at[:, cols], store_sem.at[2 + g])

    for h in range(2):
        to_near(h).wait_send()
        to_far(mine, h).wait_send()
    for kind in range(3):
        for d in range(2):
            for h in range(2):
                xs_full(kind, d, h).wait_send()
            xs_relay(kind, d).wait_send()
        for j in range(4):
            to_core(kind, j).wait_send()

    def sent_out(t, _):
        o_copy(t).wait_send()
        return 0

    lax.fori_loop(0, 8, sent_out, 0)
    z_end(0, 6, 5, 0)
    z_end(rows, 5, 6, 0)
    st_wg(0).start()
    yo().wait_recv()
    outb[...] = (o_sum[7] + yb[...]).astype(BF16)
    st_out = pltpu.make_async_copy(outb, output, store_sem.at[1])
    st_out.start()
    z_end(0, 6, 5, 1)
    z_end(rows, 5, 6, 1)
    st_wg(1).start()
    for make, where in sent:
        make(*where).wait_send()
    st_hg.wait()
    st_out.wait()
    for g in range(2):
        st_wg(g).wait()


def store(a, b, d, a_out, b_out, d_out, sems):
    pairs = ((a, a_out), (b, b_out), (d, d_out))
    copies = [pltpu.make_async_copy(s, t, sems.at[i]) for i, (s, t) in enumerate(pairs)]
    for copy in copies:
        copy.start()
    for copy in copies:
        copy.wait()


def shards(hidden, weight, cotangent):
    tok, ff = hidden.shape
    d_all = weight.shape[0]
    feat = cotangent.shape[1]
    scale = float(tok * lax.axis_size("gx")) ** (-0.5)
    any_space = pl.BlockSpec(memory_space=pl.ANY)
    sem = pltpu.SemaphoreType.DMA
    v = pltpu.VMEM
    shapes = (((tok, feat), BF16), ((tok, ff), BF16), ((feat, ff), F32))
    args = [pltpu.with_memory_space_constraint(a, pltpu.HBM) for a in (hidden, weight, cotangent)]
    results = pl.pallas_call(
        functools.partial(kernel, scale),
        out_shape=tuple(v(*shape) for shape in shapes),
        in_specs=[any_space] * 3,
        out_specs=(any_space,) * 3,
        scratch_shapes=[
            v((d_all, ff), BF16),
            v((2, tok, ff), BF16),
            v((tok, ff), BF16),
            v((24, tok, feat), BF16),
            v((8, tok, feat), F32),
            v((8, tok, feat), F32),
            v((2, 2, tok // 2, feat), F32),
            v((2, 2, tok, feat), F32),
            v((tok, feat), F32),
            v((8, feat, ff), F32),
            *(v((2, n, feat * 5 // 8, size), BF16) for n in (2, 7) for _, size in GROUPS),
            v((tok, ff), F32),
            v((tok, ff), BF16),
            v((tok, feat), BF16),
            sem((2 + WCH,)),
            sem((4,)),
            sem((2, 2)),
            sem((2, 2)),
            sem((3, 2, 3)),
            sem((3, 2, 3)),
            sem((3, 4)),
            sem((3, 4)),
            sem((2, 2, HCH)),
            sem((2, 2, HCH)),
            sem((8,)),
            sem((8,)),
            sem((2, 2, 2)),
            sem((2, 2, 2)),
            sem((1,)),
            sem((1,)),
            sem((2, 2, 7)),
            sem((2, 2, 7)),
        ],
        compiler_params=pltpu.CompilerParams(
            collective_id=0, has_side_effects=True, vmem_limit_bytes=50 * 1024 * 1024
        ),
    )(*args)
    return pl.pallas_call(
        store,
        out_shape=tuple(jax.ShapeDtypeStruct(*shape) for shape in shapes),
        in_specs=[any_space] * 3,
        out_specs=(pl.BlockSpec(memory_space=pltpu.HBM),) * 3,
        scratch_shapes=[sem((3,))],
        compiler_params=pltpu.CompilerParams(vmem_limit_bytes=1024 * 1024),
    )(*results)


def solution(mesh):
    placed = (P("gx", "gy"), P(None, "gy"), P("gx", "gy"))
    return jax.shard_map(
        shards,
        mesh=mesh,
        in_specs=placed,
        out_specs=(P("gx", "gy"), P("gx", "gy"), P("gx", "gy")),
        check_vma=False,
    )
```

```python
import functools

import jax
import jax.numpy as jnp
from jax import lax
from jax.experimental import pallas as pl
from jax.experimental.pallas import tpu as pltpu
from jax.sharding import PartitionSpec as P

MESH = pl.DeviceIdType.MESH
F32 = jnp.float32
BF16 = jnp.bfloat16
NX, NZ = 4, 8
HCH = 2
GROUPS = ((0, 512), (512, 384))
WCH = 4
ZR = 32
BOOST = 2.0**40


def zigzag(i, top):
    odd = lax.rem(i, 2)
    return top + (1 - odd) * (i // 2) - odd * ((i + 1) // 2)


def kernel(
    scale,
    hidden,
    weight,
    cotangent,
    output,
    hidden_grad,
    weight_grad,
    w,
    hid,
    hrel,
    cot,
    o_send,
    o_sum,
    xh,
    xf,
    yb,
    part,
    zs0,
    zs1,
    zb0,
    zb1,
    acc,
    hgb,
    outb,
    load_sem,
    store_sem,
    cy_s,
    cy_r,
    cx_s,
    cx_r,
    cd_s,
    cd_r,
    h_s,
    h_r,
    o_s,
    o_r,
    xo_s,
    xo_r,
    yo_s,
    yo_r,
    z_s,
    z_r,
):
    gx = lax.axis_index("gx")
    gy = lax.axis_index("gy")
    y_hi, z = gx // NZ, lax.rem(gx, NZ)
    c = lax.rem(gy, 2)
    x = lax.rem(gy // 2, NX)
    y_lo = gy // (2 * NX)
    tok, ff = hid.shape[1], hid.shape[2]
    feat = cot.shape[2]
    half = tok // 2
    rows = feat // 2

    def dev(yh, yl, xx, zz, cc):
        return (yh * NZ + zz, (yl * NX + xx) * 2 + cc)

    right, left = lax.rem(x + 1, NX), lax.rem(x + NX - 1, NX)
    across = lax.rem(x + 2, NX)
    core = dev(y_hi, y_lo, x, z, 1 - c)
    near = dev(y_hi, 1 - y_lo, x, z, c)
    far = dev(1 - y_hi, 1 - y_lo, x, z, c)
    first = dev(lax.rem(y_hi + c, 2), 1 - y_lo, x, z, c)
    second = dev(lax.rem(y_hi + 1 - c, 2), 1 - y_lo, x, z, c)
    x_dev = (dev(y_hi, y_lo, right, z, c), dev(y_hi, y_lo, left, z, c))
    z_dev = (
        dev(y_hi, y_lo, x, lax.rem(z + 1, NZ), c),
        dev(y_hi, y_lo, x, lax.rem(z + NZ - 1, NZ), c),
    )

    def rc(src, dst, ss, rs, to):
        return pltpu.make_async_remote_copy(
            src_ref=src, dst_ref=dst, send_sem=ss, recv_sem=rs, device_id=to, device_id_type=MESH
        )

    sent = []

    def go(make, *where):
        make(*where).start()
        sent.append((make, where))

    base = (y_hi * NX * 2, (1 - y_hi) * NX * 2, 16)
    middle = lax.rem(y_hi + y_lo, 2)

    def slot(kind, xx):
        return cot.at[base[kind] + xx * 2 + c]

    mine = cot.at[y_lo * NX * 2 + x * 2 + c]
    near_slot = cot.at[(1 - y_lo) * NX * 2 + x * 2 + c]
    far_slot = slot(2, x)
    ld_cot = pltpu.make_async_copy(cotangent, mine, load_sem.at[0])
    ld_hid = pltpu.make_async_copy(hidden, hid.at[0], load_sem.at[1])
    ld_cot.start()
    ld_hid.start()
    wrows = w.shape[0] // WCH
    ld_w = [
        pltpu.make_async_copy(
            weight.at[pl.ds(i * wrows, wrows)], w.at[pl.ds(i * wrows, wrows)], load_sem.at[2 + i]
        )
        for i in range(WCH)
    ]
    for copy in ld_w:
        copy.start()

    barrier = pltpu.get_barrier_semaphore()
    peers = (core, near, far, *x_dev, *z_dev)
    for peer in peers:
        pl.semaphore_signal(barrier, inc=1, device_id=peer, device_id_type=MESH)
    pl.semaphore_wait(barrier, len(peers))

    def half_of(ref, h):
        return ref.at[pl.ds(h * half, half)]

    def xs_full(kind, d, h):
        ref = half_of(slot(kind, x), h)
        return rc(ref, ref, cx_s.at[kind, d, h], cx_r.at[kind, d, h], x_dev[d])

    def xs_relay(kind, d):
        ref = half_of(slot(kind, (left, right)[d]), d)
        return rc(ref, ref, cx_s.at[kind, d, 2], cx_r.at[kind, d, 2], x_dev[d])

    def from_full(kind, d, h):
        ref = half_of(slot(kind, (left, right)[d]), h)
        return rc(ref, ref, cx_s.at[kind, d, h], cx_r.at[kind, d, h], x_dev[d])

    def from_relay(kind, d):
        ref = half_of(slot(kind, across), d)
        return rc(ref, ref, cx_s.at[kind, d, 2], cx_r.at[kind, d, 2], x_dev[d])

    def to_core(kind, j):
        ref = slot(kind, (x, left, right, across)[j])
        return rc(ref, ref, cd_s.at[kind, j], cd_r.at[kind, j], core)

    def from_core(kind, j):
        ref = cot.at[base[kind] + (x, left, right, across)[j] * 2 + 1 - c]
        return rc(ref, ref, cd_s.at[kind, j], cd_r.at[kind, j], core)

    def to_near(h):
        ref = half_of(mine, h)
        return rc(ref, ref, cy_s.at[0, h], cy_r.at[0, h], near)

    def from_near(h):
        ref = half_of(near_slot, h)
        return rc(ref, ref, cy_s.at[0, h], cy_r.at[0, h], near)

    def to_far(src, h):
        return rc(half_of(src, h), half_of(far_slot, h), cy_s.at[1, h], cy_r.at[1, h], far)

    def spread(kind, h):
        xs_full(kind, 0, h).start()
        xs_full(kind, 1, h).start()

    def relay(kind):
        for d in range(2):
            from_full(kind, d, d).wait_recv()
            xs_relay(kind, d).start()
        for d in range(2):
            from_full(kind, d, 1 - d).wait_recv()
            to_core(kind, 1 + d).start()

    def finish(kind):
        for d in range(2):
            from_relay(kind, d).wait_recv()
        to_core(kind, 3).start()

    outer, inner = pl.when(middle == 0), pl.when(middle == 1)

    ld_cot.wait()

    @outer
    def _():
        for h in range(2):
            to_near(h).start()
            spread(0, h)
        to_core(0, 0).start()

    @inner
    def _():
        for h in range(2):
            to_near(h).start()
            to_far(mine, h).start()
        spread(1, 0)
        to_core(1, 0).start()

    hrows = tok // HCH

    def hpiece(ref, g, i):
        return ref.at[pl.ds(i * hrows, hrows), pl.ds(*GROUPS[g])]

    def h_first(g, i):
        at = g, i
        return rc(hpiece(hid.at[0], g, i), hpiece(hrel, g, i), h_s.at[0, *at], h_r.at[0, *at], first)

    def h_second(g, i):
        at = g, i
        return rc(hpiece(hrel, g, i), hpiece(hid.at[1], g, i), h_s.at[1, *at], h_r.at[1, *at], second)

    def hrelay(g, i):
        h_first(g, i).wait_recv()
        go(h_second, g, i)

    ld_hid.wait()
    for i in range(HCH):
        go(h_first, 0, i)

    def out_part(t, cc):
        yp = lax.rem(y_lo + 1 + lax.rem(t, 2), 2)
        g = (yp * NX + lax.rem(x + zigzag(t // 2, 2), NX)) * 2 + cc
        wg = w[pl.ds(pl.multiple_of(g * feat, feat), feat), :]
        return lax.dot_general(hid[0], wg, (((1,), (1,)), ((), ())), preferred_element_type=F32)

    def o_copy(t):
        return rc(o_send.at[t], o_sum.at[t], o_s.at[t], o_r.at[t], core)

    def send_out(t, _):
        o_send[t] = out_part(t, 1 - c)
        o_copy(t).start()
        return 0

    def add_out(t, _):
        o_copy(t).wait_recv()
        o_sum[t] = o_sum[t] + out_part(t, c)
        return 0

    for copy in ld_w:
        copy.wait()
    lax.fori_loop(0, 6, send_out, 0)

    @outer
    def _():
        for h in range(2):
            from_near(h).wait_recv()
            to_far(near_slot, h).start()
        to_core(1, 0).start()
        relay(0)

    @inner
    def _():
        for h in range(2):
            from_near(h).wait_recv()
            spread(0, h)
            to_far(far_slot, h).wait_recv()
            spread(2, h)
        to_core(0, 0).start()
        to_core(2, 0).start()

    lax.fori_loop(6, 8, send_out, 0)
    hrelay(0, 0)

    @outer
    def _():
        to_far(far_slot, 0).wait_recv()
        spread(2, 0)
        hrelay(0, 1)
        to_far(far_slot, 1).wait_recv()
        spread(2, 1)
        for i in range(HCH):
            h_first(1, i).start()
        to_core(2, 0).start()

    @inner
    def _():
        h_first(0, 1).wait_recv()
        h_second(0, 1).start()
        for i in range(HCH):
            h_first(1, i).start()

    sent.extend((h_first, (1, i)) for i in range(HCH))
    lax.fori_loop(0, 2, add_out, 0)
    def xo_half(d, q):
        src = half_of(o_sum.at[q], d)
        return rc(src, xh.at[d, q], xo_s.at[d, q, 2], xo_r.at[d, q, 2], x_dev[d])

    def xo_full(d, q, h):
        src = half_of(o_sum.at[2 + 2 * d + q], h)
        return rc(src, half_of(xf.at[d, q], h), xo_s.at[d, q, h], xo_r.at[d, q, h], x_dev[d])

    def xo_add(q):
        for d in range(2):
            go(xo_full, d, q, 1 - d)
        for d in range(2):
            xo_half(d, q).wait_recv()
            at = 2 + 2 * d + q, pl.ds(d * half, half)
            o_sum[at] = o_sum[at] + xh[d, q]
            go(xo_full, d, q, d)

    def xo_end(q, h):
        at = pl.ds(h * half, half)
        for d in range(2):
            xo_full(d, q, h).wait_recv()
        o_sum[6 + q, at] = o_sum[6 + q, at] + xf[0, q, at] + xf[1, q, at]

    def yo(h):
        return rc(half_of(o_sum.at[6], h), half_of(yb, h), yo_s.at[h], yo_r.at[h], near)

    inner(lambda: relay(0))
    lax.fori_loop(2, 4, add_out, 0)
    relay(2)
    outer(lambda: spread(1, 0))
    spread(1, 1)
    for q in range(2):
        for d in range(2):
            go(xo_half, d, q)
    finish(0)
    hrelay(1, 0)
    lax.fori_loop(4, 6, add_out, 0)
    finish(2)
    hrelay(1, 1)

    for kind in (0, 2):
        for j in range(4):
            from_core(kind, j).wait_recv()

    def w_part(g):
        def body(i, _):
            zz = lax.rem(z + zigzag(i, 4), NZ)
            dims = (((0,), (0,)), ((), ()))
            cols = pl.ds(*GROUPS[g])
            part[i, :, cols] = lax.dot_general(
                cot[y_hi * NZ + zz], hid[0, :, cols], dims, preferred_element_type=F32
            ) + lax.dot_general(cot[16 + zz], hid[1, :, cols], dims, preferred_element_type=F32)
            return 0

        return body

    index_of = {4: 0, 3: 1, 5: 2, 2: 3, 6: 4, 1: 5, 7: 6, 0: 7}

    zs, zb = (zs0, zs1), (zb0, zb1)

    def z_rows(d, m):
        k = 4 - (m + 1) // 2
        return index_of[(k if d == 0 else -k) % NZ], ((m + d) % 2) * rows

    def z_copy(d, m, g):
        src = zs[g].at[d, m] if m < 2 else zb[g].at[d, m - 2]
        return rc(src, zb[g].at[d, m], z_s.at[g, d, m], z_r.at[g, d, m], z_dev[d])

    def bound_in(ref):
        return ref[pl.ds(rows, 8)].astype(F32)[0:1]

    def take(ref, r, unit):
        word = ref[pl.ds(r, ZR)].astype(F32)
        size = jnp.exp2(jnp.log2(jnp.maximum(jnp.abs(word), 1e-37)) * 0.125) * unit
        return jnp.where(word < 0.0, -size, size)

    def put(ref, load, bound):
        top = (bound * 1.0078125).astype(BF16)
        ref[pl.ds(rows, 8)] = jnp.broadcast_to(top, (8, top.shape[1]))
        top = top.astype(F32)
        fit = top > 1e-33
        inverse = jnp.where(fit, 32768.0 / jnp.where(fit, top, 1.0), 0.0)

        def run(r):
            v = load(r)
            u = v * inverse
            u2 = u * u
            u4 = u2 * u2
            u8 = u4 * u4
            ref[pl.ds(r, ZR)] = jnp.where(v < 0.0, -u8, u8).astype(BF16)

        in_rows(run)

    def in_rows(run):
        def body(i, _):
            run(pl.multiple_of(i * ZR, ZR))
            return 0

        lax.fori_loop(0, rows // ZR, body, 0)

    def part_rows(i, start, r, g):
        return part[i, pl.ds(start + r, ZR), pl.ds(*GROUPS[g])] * BOOST

    def peak_of(i, start, g):
        def body(n, peak):
            return jnp.maximum(peak, jnp.abs(part_rows(i, start, pl.multiple_of(n * ZR, ZR), g)))

        peak = lax.fori_loop(0, rows // ZR, body, jnp.zeros((ZR, GROUPS[g][1]), F32))
        return jnp.max(peak, axis=0, keepdims=True)

    def z_first(d, m, g):
        i, start = z_rows(d, m)
        put(zs[g].at[d, m], lambda r: part_rows(i, start, r, g), peak_of(i, start, g))
        go(z_copy, d, m, g)

    def z_one(d, m, g):
        i, start = z_rows(d, m)
        peak = peak_of(i, start, g)
        z_copy(d, m - 2, g).wait_recv()
        ref = zb[g].at[d, m - 2]
        bound = bound_in(ref)
        unit = bound * (1.0 / 32768.0)
        put(ref, lambda r: take(ref, r, unit) + part_rows(i, start, r, g), bound + peak)
        go(z_copy, d, m, g)

    def z_pair(m, g):
        z_one(0, m, g)
        z_one(1, m, g)

    def z_start(g):
        for i in range(HCH):
            h_second(g, i).wait_recv()
        run = w_part(g)
        lax.fori_loop(0, 1, run, 0)
        z_first(0, 0, g)
        z_first(1, 0, g)
        lax.fori_loop(1, 3, run, 0)
        z_first(0, 1, g)
        z_first(1, 1, g)

    def h_part(g, _):
        acc[...] = acc[...] + jnp.dot(
            cot[g], w[pl.ds(pl.multiple_of(g * feat, feat), feat), :], preferred_element_type=F32
        )
        return 0

    z_start(0)
    relay(1)
    z_start(1)
    lax.fori_loop(6, 8, add_out, 0)
    z_pair(2, 0)
    lax.fori_loop(3, 8, w_part(0), 0)
    z_pair(3, 0)
    xo_add(0)
    z_pair(2, 1)
    lax.fori_loop(3, 8, w_part(1), 0)
    z_pair(3, 1)
    finish(1)
    xo_add(1)
    for j in range(4):
        from_core(1, j).wait_recv()
    z_pair(4, 0)
    acc[...] = jnp.dot(cot[0], w[pl.ds(0, feat), :], preferred_element_type=F32)
    lax.fori_loop(1, 4, h_part, 0)
    z_pair(4, 1)
    xo_end(0, 0)
    go(yo, 0)
    lax.fori_loop(4, 9, h_part, 0)
    z_pair(5, 0)
    lax.fori_loop(9, 13, h_part, 0)
    z_pair(5, 1)
    xo_end(0, 1)
    go(yo, 1)
    lax.fori_loop(13, 16, h_part, 0)
    hgb[...] = acc[...].astype(BF16)
    st_hg = pltpu.make_async_copy(hgb, hidden_grad, store_sem.at[0])
    st_hg.start()
    z_pair(6, 0)
    z_pair(6, 1)
    xo_end(1, 0)
    xo_end(1, 1)

    def z_end(start, m0, m1, g):
        z_copy(0, m0, g).wait_recv()
        z_copy(1, m1, g).wait_recv()

        refs = zb[g].at[0, m0], zb[g].at[1, m1]
        unit0, unit1 = (bound_in(ref) * (1.0 / 32768.0) for ref in refs)

        def run(r):
            v = part_rows(7, start, r, g) + take(refs[0], r, unit0) + take(refs[1], r, unit1)
            part[7, pl.ds(start + r, ZR), pl.ds(*GROUPS[g])] = v * (scale / BOOST)

        in_rows(run)

    def st_wg(g, i):
        at = pl.ds(i * rows, rows), pl.ds(*GROUPS[g])
        return pltpu.make_async_copy(part.at[7, *at], weight_grad.at[*at], store_sem.at[2 + 2 * g + i])

    for h in range(2):
        to_near(h).wait_send()
        to_far(mine, h).wait_send()
    for kind in range(3):
        for d in range(2):
            for h in range(2):
                xs_full(kind, d, h).wait_send()
            xs_relay(kind, d).wait_send()
        for j in range(4):
            to_core(kind, j).wait_send()

    def sent_out(t, _):
        o_copy(t).wait_send()
        return 0

    lax.fori_loop(0, 8, sent_out, 0)
    z_end(0, 6, 5, 0)
    st_wg(0, 0).start()
    z_end(rows, 5, 6, 0)
    st_wg(0, 1).start()
    for h in range(2):
        yo(h).wait_recv()
    outb[...] = (o_sum[7] + yb[...]).astype(BF16)
    st_out = pltpu.make_async_copy(outb, output, store_sem.at[1])
    st_out.start()
    z_end(0, 6, 5, 1)
    st_wg(1, 0).start()
    z_end(rows, 5, 6, 1)
    st_wg(1, 1).start()
    for make, where in sent:
        make(*where).wait_send()
    st_hg.wait()
    st_out.wait()
    for g in range(2):
        for i in range(2):
            st_wg(g, i).wait()


def store(a, b, d, a_out, b_out, d_out, sems):
    pairs = ((a, a_out), (b, b_out), (d, d_out))
    copies = [pltpu.make_async_copy(s, t, sems.at[i]) for i, (s, t) in enumerate(pairs)]
    for copy in copies:
        copy.start()
    for copy in copies:
        copy.wait()


def shards(hidden, weight, cotangent):
    tok, ff = hidden.shape
    d_all = weight.shape[0]
    feat = cotangent.shape[1]
    scale = float(tok * lax.axis_size("gx")) ** (-0.5)
    any_space = pl.BlockSpec(memory_space=pl.ANY)
    sem = pltpu.SemaphoreType.DMA
    v = pltpu.VMEM
    shapes = (((tok, feat), BF16), ((tok, ff), BF16), ((feat, ff), F32))
    args = [pltpu.with_memory_space_constraint(a, pltpu.HBM) for a in (hidden, weight, cotangent)]
    results = pl.pallas_call(
        functools.partial(kernel, scale),
        out_shape=tuple(v(*shape) for shape in shapes),
        in_specs=[any_space] * 3,
        out_specs=(any_space,) * 3,
        scratch_shapes=[
            v((d_all, ff), BF16),
            v((2, tok, ff), BF16),
            v((tok, ff), BF16),
            v((24, tok, feat), BF16),
            v((8, tok, feat), F32),
            v((8, tok, feat), F32),
            v((2, 2, tok // 2, feat), F32),
            v((2, 2, tok, feat), F32),
            v((tok, feat), F32),
            v((8, feat, ff), F32),
            *(v((2, n, feat // 2 + 8, size), BF16) for n in (2, 7) for _, size in GROUPS),
            v((tok, ff), F32),
            v((tok, ff), BF16),
            v((tok, feat), BF16),
            sem((2 + WCH,)),
            sem((6,)),
            sem((2, 2)),
            sem((2, 2)),
            sem((3, 2, 3)),
            sem((3, 2, 3)),
            sem((3, 4)),
            sem((3, 4)),
            sem((2, 2, HCH)),
            sem((2, 2, HCH)),
            sem((8,)),
            sem((8,)),
            sem((2, 2, 3)),
            sem((2, 2, 3)),
            sem((2,)),
            sem((2,)),
            sem((2, 2, 7)),
            sem((2, 2, 7)),
        ],
        compiler_params=pltpu.CompilerParams(
            collective_id=0, has_side_effects=True, vmem_limit_bytes=50 * 1024 * 1024
        ),
    )(*args)
    return pl.pallas_call(
        store,
        out_shape=tuple(jax.ShapeDtypeStruct(*shape) for shape in shapes),
        in_specs=[any_space] * 3,
        out_specs=(pl.BlockSpec(memory_space=pltpu.HBM),) * 3,
        scratch_shapes=[sem((3,))],
        compiler_params=pltpu.CompilerParams(vmem_limit_bytes=1024 * 1024),
    )(*results)


def solution(mesh):
    placed = (P("gx", "gy"), P(None, "gy"), P("gx", "gy"))
    return jax.shard_map(
        shards,
        mesh=mesh,
        in_specs=placed,
        out_specs=(P("gx", "gy"), P("gx", "gy"), P("gx", "gy")),
        check_vma=False,
    )
```

```python
import functools

import jax
import jax.numpy as jnp
from jax import lax
from jax.experimental import pallas as pl
from jax.experimental.pallas import tpu as pltpu
from jax.sharding import PartitionSpec as P

MESH = pl.DeviceIdType.MESH
F32 = jnp.float32
BF16 = jnp.bfloat16
NX, NZ = 4, 8
HCH = 2
GROUPS = ((0, 512), (512, 384))
WCH = 4
ZR = 32
BOOST = 2.0**40


def zigzag(i, top):
    odd = lax.rem(i, 2)
    return top + (1 - odd) * (i // 2) - odd * ((i + 1) // 2)


def kernel(
    scale,
    hidden,
    weight,
    cotangent,
    output,
    hidden_grad,
    weight_grad,
    w,
    hid,
    hrel,
    cot,
    o_send,
    o_sum,
    xh,
    xf,
    yb,
    part,
    zs0,
    zs1,
    zb0,
    zb1,
    acc,
    hgb,
    outb,
    load_sem,
    store_sem,
    cy_s,
    cy_r,
    cx_s,
    cx_r,
    cd_s,
    cd_r,
    h_s,
    h_r,
    o_s,
    o_r,
    xo_s,
    xo_r,
    yo_s,
    yo_r,
    z_s,
    z_r,
):
    gx = lax.axis_index("gx")
    gy = lax.axis_index("gy")
    y_hi, z = gx // NZ, lax.rem(gx, NZ)
    c = lax.rem(gy, 2)
    x = lax.rem(gy // 2, NX)
    y_lo = gy // (2 * NX)
    tok, ff = hid.shape[1], hid.shape[2]
    feat = cot.shape[2]
    half = tok // 2
    rows = feat // 2

    def dev(yh, yl, xx, zz, cc):
        return (yh * NZ + zz, (yl * NX + xx) * 2 + cc)

    right, left = lax.rem(x + 1, NX), lax.rem(x + NX - 1, NX)
    across = lax.rem(x + 2, NX)
    core = dev(y_hi, y_lo, x, z, 1 - c)
    near = dev(y_hi, 1 - y_lo, x, z, c)
    far = dev(1 - y_hi, 1 - y_lo, x, z, c)
    first = dev(lax.rem(y_hi + c, 2), 1 - y_lo, x, z, c)
    second = dev(lax.rem(y_hi + 1 - c, 2), 1 - y_lo, x, z, c)
    x_dev = (dev(y_hi, y_lo, right, z, c), dev(y_hi, y_lo, left, z, c))
    z_dev = (
        dev(y_hi, y_lo, x, lax.rem(z + 1, NZ), c),
        dev(y_hi, y_lo, x, lax.rem(z + NZ - 1, NZ), c),
    )

    def rc(src, dst, ss, rs, to):
        return pltpu.make_async_remote_copy(
            src_ref=src, dst_ref=dst, send_sem=ss, recv_sem=rs, device_id=to, device_id_type=MESH
        )

    sent = []

    def go(make, *where):
        make(*where).start()
        sent.append((make, where))

    base = (y_hi * NX * 2, (1 - y_hi) * NX * 2, 16)
    middle = lax.rem(y_hi + y_lo, 2)

    def slot(kind, xx):
        return cot.at[base[kind] + xx * 2 + c]

    mine = cot.at[y_lo * NX * 2 + x * 2 + c]
    near_slot = cot.at[(1 - y_lo) * NX * 2 + x * 2 + c]
    far_slot = slot(2, x)
    ld_cot = pltpu.make_async_copy(cotangent, mine, load_sem.at[0])
    ld_hid = pltpu.make_async_copy(hidden, hid.at[0], load_sem.at[1])
    ld_cot.start()
    ld_hid.start()
    wrows = w.shape[0] // WCH
    ld_w = [
        pltpu.make_async_copy(
            weight.at[pl.ds(i * wrows, wrows)], w.at[pl.ds(i * wrows, wrows)], load_sem.at[2 + i]
        )
        for i in range(WCH)
    ]
    for copy in ld_w:
        copy.start()

    barrier = pltpu.get_barrier_semaphore()
    peers = (core, near, far, *x_dev, *z_dev)
    for peer in peers:
        pl.semaphore_signal(barrier, inc=1, device_id=peer, device_id_type=MESH)
    pl.semaphore_wait(barrier, len(peers))

    def half_of(ref, h):
        return ref.at[pl.ds(h * half, half)]

    def xs_full(kind, d, h):
        ref = half_of(slot(kind, x), h)
        return rc(ref, ref, cx_s.at[kind, d, h], cx_r.at[kind, d, h], x_dev[d])

    def xs_relay(kind, d):
        ref = half_of(slot(kind, (left, right)[d]), d)
        return rc(ref, ref, cx_s.at[kind, d, 2], cx_r.at[kind, d, 2], x_dev[d])

    def from_full(kind, d, h):
        ref = half_of(slot(kind, (left, right)[d]), h)
        return rc(ref, ref, cx_s.at[kind, d, h], cx_r.at[kind, d, h], x_dev[d])

    def from_relay(kind, d):
        ref = half_of(slot(kind, across), d)
        return rc(ref, ref, cx_s.at[kind, d, 2], cx_r.at[kind, d, 2], x_dev[d])

    def to_core(kind, j):
        ref = slot(kind, (x, left, right, across)[j])
        return rc(ref, ref, cd_s.at[kind, j], cd_r.at[kind, j], core)

    def from_core(kind, j):
        ref = cot.at[base[kind] + (x, left, right, across)[j] * 2 + 1 - c]
        return rc(ref, ref, cd_s.at[kind, j], cd_r.at[kind, j], core)

    def to_near(h):
        ref = half_of(mine, h)
        return rc(ref, ref, cy_s.at[0, h], cy_r.at[0, h], near)

    def from_near(h):
        ref = half_of(near_slot, h)
        return rc(ref, ref, cy_s.at[0, h], cy_r.at[0, h], near)

    def to_far(src, h):
        return rc(half_of(src, h), half_of(far_slot, h), cy_s.at[1, h], cy_r.at[1, h], far)

    def spread(kind, h):
        xs_full(kind, 0, h).start()
        xs_full(kind, 1, h).start()

    def relay(kind):
        for d in range(2):
            from_full(kind, d, d).wait_recv()
            xs_relay(kind, d).start()
        for d in range(2):
            from_full(kind, d, 1 - d).wait_recv()
            to_core(kind, 1 + d).start()

    def finish(kind):
        for d in range(2):
            from_relay(kind, d).wait_recv()
        to_core(kind, 3).start()

    outer, inner = pl.when(middle == 0), pl.when(middle == 1)

    ld_cot.wait()

    @outer
    def _():
        for h in range(2):
            to_near(h).start()
            spread(0, h)
        to_core(0, 0).start()

    @inner
    def _():
        for h in range(2):
            to_near(h).start()
            to_far(mine, h).start()
        spread(1, 0)
        to_core(1, 0).start()

    hrows = tok // HCH

    def hpiece(ref, g, i):
        return ref.at[pl.ds(i * hrows, hrows), pl.ds(*GROUPS[g])]

    def h_first(g, i):
        at = g, i
        return rc(hpiece(hid.at[0], g, i), hpiece(hrel, g, i), h_s.at[0, *at], h_r.at[0, *at], first)

    def h_second(g, i):
        at = g, i
        return rc(hpiece(hrel, g, i), hpiece(hid.at[1], g, i), h_s.at[1, *at], h_r.at[1, *at], second)

    def hrelay(g, i):
        h_first(g, i).wait_recv()
        go(h_second, g, i)

    ld_hid.wait()
    for i in range(HCH):
        go(h_first, 0, i)

    def out_part(t, cc):
        yp = lax.rem(y_lo + 1 + lax.rem(t, 2), 2)
        g = (yp * NX + lax.rem(x + zigzag(t // 2, 2), NX)) * 2 + cc
        wg = w[pl.ds(pl.multiple_of(g * feat, feat), feat), :]
        return lax.dot_general(hid[0], wg, (((1,), (1,)), ((), ())), preferred_element_type=F32)

    def o_copy(t):
        return rc(o_send.at[t], o_sum.at[t], o_s.at[t], o_r.at[t], core)

    def send_out(t, _):
        o_send[t] = out_part(t, 1 - c)
        o_copy(t).start()
        return 0

    def add_out(t, _):
        o_copy(t).wait_recv()
        o_sum[t] = o_sum[t] + out_part(t, c)
        return 0

    for copy in ld_w:
        copy.wait()
    lax.fori_loop(0, 6, send_out, 0)

    @outer
    def _():
        for h in range(2):
            from_near(h).wait_recv()
            to_far(near_slot, h).start()
        to_core(1, 0).start()
        relay(0)

    @inner
    def _():
        for h in range(2):
            from_near(h).wait_recv()
            spread(0, h)
            to_far(far_slot, h).wait_recv()
            spread(2, h)
        to_core(0, 0).start()
        to_core(2, 0).start()

    lax.fori_loop(6, 8, send_out, 0)
    hrelay(0, 0)

    @outer
    def _():
        to_far(far_slot, 0).wait_recv()
        spread(2, 0)
        hrelay(0, 1)
        to_far(far_slot, 1).wait_recv()
        spread(2, 1)
        for i in range(HCH):
            h_first(1, i).start()
        to_core(2, 0).start()

    @inner
    def _():
        h_first(0, 1).wait_recv()
        h_second(0, 1).start()
        for i in range(HCH):
            h_first(1, i).start()

    sent.extend((h_first, (1, i)) for i in range(HCH))
    lax.fori_loop(0, 2, add_out, 0)
    def xo_half(d, q):
        src = half_of(o_sum.at[q], d)
        return rc(src, xh.at[d, q], xo_s.at[d, q, 2], xo_r.at[d, q, 2], x_dev[d])

    def xo_full(d, q, h):
        src = half_of(o_sum.at[2 + 2 * d + q], h)
        return rc(src, half_of(xf.at[d, q], h), xo_s.at[d, q, h], xo_r.at[d, q, h], x_dev[d])

    def xo_add(q):
        for d in range(2):
            go(xo_full, d, q, 1 - d)
        for d in range(2):
            xo_half(d, q).wait_recv()
            at = 2 + 2 * d + q, pl.ds(d * half, half)
            o_sum[at] = o_sum[at] + xh[d, q]
            go(xo_full, d, q, d)

    def xo_end(q, h):
        at = pl.ds(h * half, half)
        for d in range(2):
            xo_full(d, q, h).wait_recv()
        o_sum[6 + q, at] = o_sum[6 + q, at] + xf[0, q, at] + xf[1, q, at]

    def yo(h):
        return rc(half_of(o_sum.at[6], h), half_of(yb, h), yo_s.at[h], yo_r.at[h], near)

    inner(lambda: relay(0))
    lax.fori_loop(2, 4, add_out, 0)
    relay(2)
    outer(lambda: spread(1, 0))
    spread(1, 1)
    for q in range(2):
        for d in range(2):
            go(xo_half, d, q)
    finish(0)
    hrelay(1, 0)
    lax.fori_loop(4, 6, add_out, 0)
    finish(2)
    hrelay(1, 1)

    for kind in (0, 2):
        for j in range(4):
            from_core(kind, j).wait_recv()

    def w_part(g):
        def body(i, _):
            zz = lax.rem(z + zigzag(i, 4), NZ)
            dims = (((0,), (0,)), ((), ()))
            cols = pl.ds(*GROUPS[g])
            part[i, :, cols] = lax.dot_general(
                cot[y_hi * NZ + zz], hid[0, :, cols], dims, preferred_element_type=F32
            ) + lax.dot_general(cot[16 + zz], hid[1, :, cols], dims, preferred_element_type=F32)
            return 0

        return body

    index_of = {4: 0, 3: 1, 5: 2, 2: 3, 6: 4, 1: 5, 7: 6, 0: 7}

    zs, zb = (zs0, zs1), (zb0, zb1)

    def z_rows(d, m):
        k = 4 - (m + 1) // 2
        return index_of[(k if d == 0 else -k) % NZ], ((m + d) % 2) * rows

    def z_copy(d, m, g):
        src = zs[g].at[d, m] if m < 2 else zb[g].at[d, m - 2]
        return rc(src, zb[g].at[d, m], z_s.at[g, d, m], z_r.at[g, d, m], z_dev[d])

    def bound_in(ref):
        return ref[pl.ds(rows, 8)].astype(F32)[0:1]

    def take(ref, r, unit):
        word = ref[pl.ds(r, ZR)].astype(F32)
        size = jnp.exp2(jnp.log2(jnp.maximum(jnp.abs(word), 1e-37)) * 0.125) * unit
        return jnp.where(word < 0.0, -size, size)

    def put(ref, load, bound):
        top = (bound * 1.0078125).astype(BF16)
        ref[pl.ds(rows, 8)] = jnp.broadcast_to(top, (8, top.shape[1]))
        top = top.astype(F32)
        fit = top > 1e-33
        inverse = jnp.where(fit, 32768.0 / jnp.where(fit, top, 1.0), 0.0)

        def run(r):
            v = load(r)
            u = v * inverse
            u2 = u * u
            u4 = u2 * u2
            u8 = u4 * u4
            ref[pl.ds(r, ZR)] = jnp.where(v < 0.0, -u8, u8).astype(BF16)

        in_rows(run)

    def in_rows(run):
        def body(i, _):
            run(pl.multiple_of(i * ZR, ZR))
            return 0

        lax.fori_loop(0, rows // ZR, body, 0)

    def part_rows(i, start, r, g):
        return part[i, pl.ds(start + r, ZR), pl.ds(*GROUPS[g])] * BOOST

    def peak_of(i, start, g):
        def body(n, peak):
            return jnp.maximum(peak, jnp.abs(part_rows(i, start, pl.multiple_of(n * ZR, ZR), g)))

        peak = lax.fori_loop(0, rows // ZR, body, jnp.zeros((ZR, GROUPS[g][1]), F32))
        return jnp.max(peak, axis=0, keepdims=True)

    def z_first(d, m, g):
        i, start = z_rows(d, m)
        put(zs[g].at[d, m], lambda r: part_rows(i, start, r, g), peak_of(i, start, g))
        go(z_copy, d, m, g)

    def z_one(d, m, g):
        i, start = z_rows(d, m)
        peak = peak_of(i, start, g)
        z_copy(d, m - 2, g).wait_recv()
        ref = zb[g].at[d, m - 2]
        bound = bound_in(ref)
        unit = bound * (1.0 / 32768.0)
        put(ref, lambda r: take(ref, r, unit) + part_rows(i, start, r, g), bound + peak)
        go(z_copy, d, m, g)

    def z_pair(m, g):
        z_one(0, m, g)
        z_one(1, m, g)

    def z_start(g):
        for i in range(HCH):
            h_second(g, i).wait_recv()
        run = w_part(g)
        lax.fori_loop(0, 1, run, 0)
        z_first(0, 0, g)
        z_first(1, 0, g)
        lax.fori_loop(1, 3, run, 0)
        z_first(0, 1, g)
        z_first(1, 1, g)

    def h_part(g, _):
        acc[...] = acc[...] + jnp.dot(
            cot[g], w[pl.ds(pl.multiple_of(g * feat, feat), feat), :], preferred_element_type=F32
        )
        return 0

    z_start(0)
    relay(1)
    z_start(1)
    lax.fori_loop(6, 8, add_out, 0)
    z_pair(2, 0)
    lax.fori_loop(3, 8, w_part(0), 0)
    z_pair(3, 0)
    xo_add(0)
    z_pair(2, 1)
    lax.fori_loop(3, 8, w_part(1), 0)
    z_pair(3, 1)
    finish(1)
    xo_add(1)
    for j in range(4):
        from_core(1, j).wait_recv()
    z_pair(4, 0)
    acc[...] = jnp.dot(cot[0], w[pl.ds(0, feat), :], preferred_element_type=F32)
    lax.fori_loop(1, 4, h_part, 0)
    z_pair(5, 0)
    z_pair(4, 1)
    xo_end(0, 0)
    go(yo, 0)
    lax.fori_loop(4, 8, h_part, 0)
    z_pair(5, 1)
    z_pair(6, 0)
    xo_end(0, 1)
    go(yo, 1)
    lax.fori_loop(8, 12, h_part, 0)
    z_pair(6, 1)
    lax.fori_loop(12, 16, h_part, 0)
    hgb[...] = acc[...].astype(BF16)
    st_hg = pltpu.make_async_copy(hgb, hidden_grad, store_sem.at[0])
    st_hg.start()
    xo_end(1, 0)
    xo_end(1, 1)

    def z_end(start, m0, m1, g):
        z_copy(0, m0, g).wait_recv()
        z_copy(1, m1, g).wait_recv()

        refs = zb[g].at[0, m0], zb[g].at[1, m1]
        unit0, unit1 = (bound_in(ref) * (1.0 / 32768.0) for ref in refs)

        def run(r):
            v = part_rows(7, start, r, g) + take(refs[0], r, unit0) + take(refs[1], r, unit1)
            part[7, pl.ds(start + r, ZR), pl.ds(*GROUPS[g])] = v * (scale / BOOST)

        in_rows(run)

    def st_wg(g, i):
        at = pl.ds(i * rows, rows), pl.ds(*GROUPS[g])
        return pltpu.make_async_copy(part.at[7, *at], weight_grad.at[*at], store_sem.at[2 + 2 * g + i])

    for h in range(2):
        to_near(h).wait_send()
        to_far(mine, h).wait_send()
    for kind in range(3):
        for d in range(2):
            for h in range(2):
                xs_full(kind, d, h).wait_send()
            xs_relay(kind, d).wait_send()
        for j in range(4):
            to_core(kind, j).wait_send()

    def sent_out(t, _):
        o_copy(t).wait_send()
        return 0

    lax.fori_loop(0, 8, sent_out, 0)
    z_end(0, 6, 5, 0)
    st_wg(0, 0).start()
    z_end(rows, 5, 6, 0)
    st_wg(0, 1).start()
    for h in range(2):
        yo(h).wait_recv()
    outb[...] = (o_sum[7] + yb[...]).astype(BF16)
    st_out = pltpu.make_async_copy(outb, output, store_sem.at[1])
    st_out.start()
    z_end(0, 6, 5, 1)
    st_wg(1, 0).start()
    z_end(rows, 5, 6, 1)
    st_wg(1, 1).start()
    for make, where in sent:
        make(*where).wait_send()
    st_hg.wait()
    st_out.wait()
    for g in range(2):
        for i in range(2):
            st_wg(g, i).wait()


def store(a, b, d, a_out, b_out, d_out, sems):
    pairs = ((a, a_out), (b, b_out), (d, d_out))
    copies = [pltpu.make_async_copy(s, t, sems.at[i]) for i, (s, t) in enumerate(pairs)]
    for copy in copies:
        copy.start()
    for copy in copies:
        copy.wait()


def shards(hidden, weight, cotangent):
    tok, ff = hidden.shape
    d_all = weight.shape[0]
    feat = cotangent.shape[1]
    scale = float(tok * lax.axis_size("gx")) ** (-0.5)
    any_space = pl.BlockSpec(memory_space=pl.ANY)
    sem = pltpu.SemaphoreType.DMA
    v = pltpu.VMEM
    shapes = (((tok, feat), BF16), ((tok, ff), BF16), ((feat, ff), F32))
    args = [pltpu.with_memory_space_constraint(a, pltpu.HBM) for a in (hidden, weight, cotangent)]
    results = pl.pallas_call(
        functools.partial(kernel, scale),
        out_shape=tuple(v(*shape) for shape in shapes),
        in_specs=[any_space] * 3,
        out_specs=(any_space,) * 3,
        scratch_shapes=[
            v((d_all, ff), BF16),
            v((2, tok, ff), BF16),
            v((tok, ff), BF16),
            v((24, tok, feat), BF16),
            v((8, tok, feat), F32),
            v((8, tok, feat), F32),
            v((2, 2, tok // 2, feat), F32),
            v((2, 2, tok, feat), F32),
            v((tok, feat), F32),
            v((8, feat, ff), F32),
            *(v((2, n, feat // 2 + 8, size), BF16) for n in (2, 7) for _, size in GROUPS),
            v((tok, ff), F32),
            v((tok, ff), BF16),
            v((tok, feat), BF16),
            sem((2 + WCH,)),
            sem((6,)),
            sem((2, 2)),
            sem((2, 2)),
            sem((3, 2, 3)),
            sem((3, 2, 3)),
            sem((3, 4)),
            sem((3, 4)),
            sem((2, 2, HCH)),
            sem((2, 2, HCH)),
            sem((8,)),
            sem((8,)),
            sem((2, 2, 3)),
            sem((2, 2, 3)),
            sem((2,)),
            sem((2,)),
            sem((2, 2, 7)),
            sem((2, 2, 7)),
        ],
        compiler_params=pltpu.CompilerParams(
            collective_id=0, has_side_effects=True, vmem_limit_bytes=50 * 1024 * 1024
        ),
    )(*args)
    return pl.pallas_call(
        store,
        out_shape=tuple(jax.ShapeDtypeStruct(*shape) for shape in shapes),
        in_specs=[any_space] * 3,
        out_specs=(pl.BlockSpec(memory_space=pltpu.HBM),) * 3,
        scratch_shapes=[sem((3,))],
        compiler_params=pltpu.CompilerParams(vmem_limit_bytes=1024 * 1024),
    )(*results)


def solution(mesh):
    placed = (P("gx", "gy"), P(None, "gy"), P("gx", "gy"))
    return jax.shard_map(
        shards,
        mesh=mesh,
        in_specs=placed,
        out_specs=(P("gx", "gy"), P("gx", "gy"), P("gx", "gy")),
        check_vma=False,
    )
```
